128 devices in a mesh: member: 8 (over y_hi, z), lat: 16 (over y_lo, x, core).
Axes of the slice: x: 4, y: 4 (y_hi: 2, y_lo: 2; y = y_hi * 2 + y_lo), z: 4, core: 2. Of those that a mesh axis runs over, the one named last changes fastest.
Arguments:
- ensemble_state: float32 [3, 512, 128, 256], P(None, 'member', 'lat'), may hold values from -6 to 6
- obs_cell: int32 [16, 8, 256], replicated, may hold values from 0 to 255
- obs_value: float32 [16, 8, 256], replicated, may hold values from -6 to 6
- obs_prec: float32 [16, 8, 256], replicated, may hold values from 0.5 to 4
Outputs:
- analysis_a: float32 [3, 512, 128, 256], P(None, 'member', 'lat')
The draws below stay inside these ranges and needn't reach their ends.
Inputs may be any that keep to these rules, and one draw needn't show every extreme that they name: `obs_cell`: each entry is a cell of its patch of 8 by 32 cells, counted row by row.
All inputs are finite; a program needn't handle non-finite values.
Results may differ from the reference program's by a relative error of at most 0.0003.
Values sent between devices are 32-bit elements; how exact they have to be, the bound alone decides.
A program may use at most 128 MiB of HBM per device.

```python
import math
import jax
import jax.numpy as jnp
from jax import lax

BAND_GRID_ROWS = 8
NLON = 256
OBS_P = 256
ITERS = 12
STEPS = 2
ENSEMBLE_SIZE = 512
NLAT = 128
PLON = 32
N_MEMBER = 8
N_LAT = 16


def place_ends(values, stream_key, least, high):
    place = [jax.random.randint(jax.random.fold_in(stream_key, axis), (), 0, length) for axis, length in enumerate(values.shape)]
    main_axis = values.shape.index(max(values.shape))
    next_to = place[:main_axis] + [(place[main_axis] + 1) % values.shape[main_axis]] + place[main_axis + 1:]
    return values.at[tuple(place)].set(least).at[tuple(next_to)].set(high)


def levels(own_key, dims, shards, smallest, largest):
    def one(axis_at, blocks):
        draws = jax.random.uniform(jax.random.fold_in(jax.random.fold_in(own_key, 6), axis_at), (blocks,), jnp.float32, smallest / len(shards), largest / len(shards))
        return jnp.repeat(jnp.exp(draws), dims[axis_at] // blocks).reshape((-1,) + (1,) * (len(dims) - axis_at - 1))

    loudness = one(*shards[0])
    for cut in shards[1:]:
        loudness = loudness * one(*cut)
    return loudness


def noise(stream_key, dims, scale, most, cuts=(), held_as=jnp.bfloat16):
    level = levels(stream_key, dims, cuts, -0.22, 0.18) if cuts else 1.0
    entries = jax.random.normal(stream_key, dims, jnp.float32) * scale * level
    return jnp.minimum(jnp.maximum(entries, -most), most).astype(held_as)


def setup_inputs(seed: int = 0) -> dict:
    arg_keys = jax.random.split(jax.random.key(seed), 5)
    ensemble_state = noise(arg_keys[0], (3, ENSEMBLE_SIZE, NLAT, NLON), 1.0, 6.0, ((1, 8), (2, 16)), jnp.float32)
    obs_cell = place_ends(jax.random.randint(arg_keys[1], (N_LAT, N_MEMBER, OBS_P), 0, BAND_GRID_ROWS * PLON), jax.random.fold_in(arg_keys[1], 1), 0, (BAND_GRID_ROWS * PLON) - 1).astype(jnp.int32)
    obs_value = noise(arg_keys[2], (N_LAT, N_MEMBER, OBS_P), 1.0, 6.0, (), jnp.float32)
    obs_prec = jnp.clip(jnp.exp(jax.random.uniform(arg_keys[3], (N_LAT, N_MEMBER, OBS_P), jnp.float32, math.log(0.5), math.log(4.0))), 0.5, 4.0)
    return dict(ensemble_state=ensemble_state, obs_cell=obs_cell, obs_value=obs_value, obs_prec=obs_prec)


time_step = 0.3
coriolis_base = 0.5
coriolis_slope = 1.0

def planetary(row_ids, total_rows):
    return coriolis_base + coriolis_slope * (row_ids / total_rows - 0.5)

def along_lon(model_field):
    inner = jnp.pad(model_field[:, 1:-1, :], ((0, 0), (0, 0), (1, 1)))
    return 0.5 * (inner[:, :, 2:] - inner[:, :, :-2])

def along_lat(model_field):
    return 0.5 * (model_field[:, 2:, :] - model_field[:, :-2, :])

def tendency(padded, spinup_rows):
    height, zonal, meridional = (padded[0], padded[1], padded[2])
    spin = spinup_rows[None, :, None]
    height_rate = -(along_lon(zonal) + along_lat(meridional))
    zonal_rate = -along_lon(height) + spin * meridional[:, 1:-1, :]
    merid_rate = -along_lat(height) - spin * zonal[:, 1:-1, :]
    return jnp.stack([height_rate, zonal_rate, merid_rate])

def advance_model(model_state, spinup_rows, widen_band):
    for sweep in range(STEPS):
        first_rate = tendency(widen_band(model_state), spinup_rows)
        midpoint = model_state + time_step * first_rate
        second_rate = tendency(widen_band(midpoint), spinup_rows)
        model_state = model_state + 0.5 * time_step * (first_rate + second_rate)
    return model_state

def analyse(blocks, near_values, near_precs, near_cells, states, lat_index, lon_index, section_width, band_rows):
    members = blocks.shape[2]
    highest = lax.Precision.HIGHEST
    offsets = jnp.arange(3, dtype=jnp.int32) - 1
    obs_mean = lax.optimization_barrier(jnp.mean(blocks, axis=2))
    deviation = blocks - obs_mean[:, :, None, :]
    innovation = near_values - obs_mean
    obs_row = (offsets[:, None, None] * band_rows + near_cells // section_width).astype(jnp.float32)
    obs_col = (offsets[None, :, None] * section_width + near_cells % section_width).astype(jnp.float32)
    north = (obs_row - 0.5 * (band_rows - 1)) / band_rows
    east = (obs_col - 0.5 * (section_width - 1)) / section_width
    taper = jnp.exp(-0.5 * (north * north + east * east))
    weight = near_precs * taper
    scaled = deviation * weight[:, :, None, :]
    identity = jnp.eye(members, dtype=jnp.float32)
    gram_matrix = jnp.einsum('abko,abjo->kj', scaled, deviation, precision=highest) + (members - 1.0) * identity
    drive_vec = jnp.einsum('abko,abo->k', scaled, innovation, precision=highest)
    fro_norm = jnp.sqrt(jnp.sum(gram_matrix * gram_matrix))
    root_iter = gram_matrix / fro_norm
    inverse = identity
    for sweep in range(ITERS):
        correction = 1.5 * identity - 0.5 * jnp.dot(inverse, root_iter, precision=highest)
        root_iter = jnp.dot(root_iter, correction, precision=highest)
        inverse = jnp.dot(correction, inverse, precision=highest)
    mean_weight = jnp.dot(inverse, jnp.dot(inverse, drive_vec, precision=highest), precision=highest) / fro_norm
    weights = jnp.sqrt(members - 1.0) / jnp.sqrt(fro_norm) * inverse + mean_weight[:, None]
    state_mean = lax.optimization_barrier(jnp.mean(states, axis=1, keepdims=True))
    return state_mean + jnp.einsum('jk,fjc->fkc', weights, states - state_mean, precision=highest)

def reference(ensemble_state, obs_cell, obs_value, obs_prec):
    section_width = NLON // N_MEMBER
    spinup_rows = planetary(jnp.arange(NLAT, dtype=jnp.float32), NLAT)

    def widen_band(model_field):
        return jnp.pad(model_field, ((0, 0), (0, 0), (1, 1), (0, 0)))
    advance_model_alt = advance_model(ensemble_state, spinup_rows, widen_band)
    local_patches = advance_model_alt.reshape(3, ENSEMBLE_SIZE, N_LAT, BAND_GRID_ROWS, N_MEMBER, section_width)
    local_patches = local_patches.transpose(2, 4, 0, 1, 3, 5).reshape(N_LAT, N_MEMBER, 3, ENSEMBLE_SIZE, BAND_GRID_ROWS * section_width)
    heights = local_patches[:, :, 0]
    where_obs = jnp.broadcast_to(obs_cell[:, :, None, :], (N_LAT, N_MEMBER, ENSEMBLE_SIZE, OBS_P))
    observed = jnp.take_along_axis(heights, where_obs, axis=3)
    padded_obs = jnp.pad(observed, ((1, 1), (1, 1), (0, 0), (0, 0)))
    padded_values = jnp.pad(obs_value, ((1, 1), (1, 1), (0, 0)))
    padded_precs = jnp.pad(obs_prec, ((1, 1), (1, 1), (0, 0)))
    padded_cells = jnp.pad(obs_cell, ((1, 1), (1, 1), (0, 0)))

    def analyse_patch(patch_id):
        zero_index = jnp.zeros((), jnp.int32)
        lat_index = (patch_id // N_MEMBER).astype(jnp.int32)
        lon_index = (patch_id % N_MEMBER).astype(jnp.int32)
        blocks = lax.dynamic_slice(padded_obs, (lat_index, lon_index, zero_index, zero_index), (3, 3, ENSEMBLE_SIZE, OBS_P))
        near_values = lax.dynamic_slice(padded_values, (lat_index, lon_index, zero_index), (3, 3, OBS_P))
        near_precs = lax.dynamic_slice(padded_precs, (lat_index, lon_index, zero_index), (3, 3, OBS_P))
        near_cells = lax.dynamic_slice(padded_cells, (lat_index, lon_index, zero_index), (3, 3, OBS_P))
        states = local_patches[lat_index, lon_index]
        return analyse(blocks, near_values, near_precs, near_cells, states, lat_index, lon_index, section_width, BAND_GRID_ROWS)
    analysed = lax.map(analyse_patch, jnp.arange(N_LAT * N_MEMBER, dtype=jnp.int32))
    analysed = analysed.reshape(N_LAT, N_MEMBER, 3, ENSEMBLE_SIZE, BAND_GRID_ROWS, section_width)
    analysis_a = analysed.transpose(2, 3, 0, 4, 1, 5).reshape(3, ENSEMBLE_SIZE, NLAT, NLON)
    return analysis_a
```

```python
import math

import jax
import jax.numpy as jnp
from jax import lax
from jax.experimental import pallas as pl
from jax.experimental.pallas import tpu as pltpu
from jax.sharding import PartitionSpec as P

MESH = pl.DeviceIdType.MESH
F32 = jnp.float32
BF16 = jnp.bfloat16
NM = 8
NL = 16
ENS = 512
LOC = 64
ROWS = 8
LON = 256
CELLS = 256
DT = 0.3
NN = (((1,), (0,)), ((), ()))
NT = (((1,), (1,)), ((), ()))
BLOCKS = ((0, 0), (0, 1), (1, 1))


def dot(a, b, dims=NN):
    return lax.dot_general(a, b, dims, preferred_element_type=F32)


def split(v):
    high = v.astype(BF16)
    low = (v - high.astype(F32)).astype(BF16)
    return high, low


def iota(shape, dim):
    return lax.broadcasted_iota(jnp.int32, shape, dim)


def exchange_lanes(v, halves, evens):
    a0 = jnp.where(halves, v[0], pltpu.roll(v[2], 64, 1))
    a2 = jnp.where(halves, pltpu.roll(v[0], 64, 1), v[2])
    a1 = jnp.where(halves, v[1], pltpu.roll(v[3], 64, 1))
    a3 = jnp.where(halves, pltpu.roll(v[1], 64, 1), v[3])
    o0 = jnp.where(evens, a0, pltpu.roll(a1, 32, 1))
    o1 = jnp.where(evens, pltpu.roll(a0, 96, 1), a1)
    o2 = jnp.where(evens, a2, pltpu.roll(a3, 32, 1))
    o3 = jnp.where(evens, pltpu.roll(a2, 96, 1), a3)
    return [o0, o1, o2, o3]


def row_times(row, mat_h, mat_l, dims=NN):
    high = row.astype(BF16).astype(F32)
    lhs = jnp.concatenate([high, row - high, jnp.zeros((6, row.shape[1]), F32)], axis=0)
    lhs = lhs.astype(BF16)
    first = dot(lhs, mat_h, dims)
    second = dot(lhs, mat_l, dims)
    return first[0:1] + first[1:2] + second[0:1]


def kernel(
    xs, cell, val, prec, out,
    ht, hb, pk, rh, xf, sh, sl, g0, gs, gr, ds_, dr, co,
    yh, yl, zh, zl, mh, ml, bh, bl, qh, ql, gh, gl, mf, rf,
    xh, xl, ao, ro,
    h_send, h_recv, o_send, o_recv, f_send, f_recv, g_send, g_recv, a_send, a_recv,
):
    me = lax.axis_index("member")
    lat = lax.axis_index("lat")
    south = lax.rem(lat + 1, NL)
    north = lax.rem(lat + NL - 1, NL)

    def peer(k):
        return lax.rem(me + k, NM)

    def source(k):
        return lax.rem(me + NM - k, NM)

    barrier = pltpu.get_barrier_semaphore()
    for k in range(1, NM):
        pl.semaphore_signal(barrier, inc=1, device_id={"member": peer(k)}, device_id_type=MESH)
    for there in (north, south):
        pl.semaphore_signal(barrier, inc=1, device_id={"lat": there}, device_id_type=MESH)
    pl.semaphore_wait(barrier, NM + 1)

    def halo(side, g):
        rows = pl.ds(pl.multiple_of(g * 8, 8), 8)
        src = xs.at[:, 0:4, rows, :] if side == 0 else xs.at[:, 4:8, rows, :]
        dst = (hb if side == 0 else ht).at[:, :, rows, :]
        return pltpu.make_async_remote_copy(
            src_ref=src, dst_ref=dst, send_sem=h_send.at[side, g], recv_sem=h_recv.at[side, g],
            device_id={"lat": north if side == 0 else south}, device_id_type=MESH,
        )

    @pl.loop(0, 8)
    def _(g):
        halo(0, g).start()
        halo(1, g).start()

    cells_at = iota((CELLS, CELLS), 0)
    for b in range(3):
        q = me + (b - 1)
        q_in = jnp.clip(q, 0, NM - 1)
        there = ((q >= 0) & (q < NM)).astype(jnp.int32).astype(F32)
        c_row = cell[lat, pl.ds(q_in, 1), :]
        p_row = prec[lat, pl.ds(q_in, 1), :] * there
        v_row = val[lat, pl.ds(q_in, 1), :] * p_row
        parts = []
        for r in (p_row, v_row):
            one = r.astype(BF16).astype(F32)
            two = (r - one).astype(BF16).astype(F32)
            parts += [one, two, r - one - two]
        lhs = jnp.concatenate(parts + [jnp.zeros((2, CELLS), F32)], axis=0).astype(BF16)
        hot = jnp.where(cells_at == c_row, 1.0, 0.0).astype(BF16)
        sums = dot(lhs, hot, NT)
        p_sum = sums[0:1] + sums[1:2] + sums[2:3]
        v_sum = sums[3:4] + sums[4:5] + sums[5:6]
        root = jnp.sqrt(p_sum)
        co[b, 0:1, :] = root
        co[b, 1:2, :] = jnp.where(p_sum > 0.0, v_sum / jnp.where(p_sum > 0.0, root, 1.0), 0.0)

    lane = iota((8, LON), 1)
    west_edge = lane == 0
    east_edge = lane == LON - 1
    lane1 = iota((8, 128), 1)
    halves = lane1 < 64
    evens = (lane1 & 32) == 0
    in_north = jnp.minimum(lat, 1).astype(F32)
    in_south = jnp.minimum(NL - 1 - lat, 1).astype(F32)

    def mask_row(r, state):
        if r < 0:
            return [s * in_north for s in state]
        if r >= ROWS:
            return [s * in_south for s in state]
        return state

    def slope(q):
        east = jnp.where(east_edge, 0.0, pltpu.roll(q, LON - 1, 1))
        west = jnp.where(west_edge, 0.0, pltpu.roll(q, 1, 1))
        return east - west

    half = 0.5 * DT

    def euler(states, r):
        h, u, v = states[r]
        above, below = states[r - 1], states[r + 1]
        spin = DT * (0.5 + ((lat * ROWS + r).astype(F32) * (1.0 / (NL * ROWS)) - 0.5))
        nh = h - half * (slope(u) + (below[2] - above[2]))
        nu = u - half * slope(h) + spin * v
        nv = v - half * (below[0] - above[0]) - spin * u
        return mask_row(r, [nh, nu, nv])

    for f in range(3):
        pk[f, 0, :, :] = jnp.zeros((LOC, CELLS), F32)
        pk[f, 9, :, :] = jnp.zeros((LOC, CELLS), F32)

    def obs_copy(g, k, mine):
        d = peer(k)
        src = pk.at[0, pl.ds(d, 3), pl.ds(pl.multiple_of(g * 8, 8), 8), :]
        owner = me if mine else source(k)
        dst = rh.at[:, pl.ds(pl.multiple_of(owner * LOC + g * 8, 8), 8), :]
        return pltpu.make_async_remote_copy(
            src_ref=src, dst_ref=dst, send_sem=o_send.at[g, k], recv_sem=o_recv.at[g, k],
            device_id={"member": d}, device_id_type=MESH,
        )

    far_first = (4, 2, 6, 3, 5, 1, 7)

    @pl.loop(0, 8)
    def _(g):
        halo(0, g).wait_recv()
        halo(1, g).wait_recv()
        rows = pl.ds(pl.multiple_of(g * 8, 8), 8)

        def start_row(r):
            if r < 0:
                vals = [ht[f, r + 4, rows, :] for f in range(3)]
            elif r >= ROWS:
                vals = [hb[f, r - ROWS, rows, :] for f in range(3)]
            else:
                vals = [xs[f, r, rows, :] for f in range(3)]
            return mask_row(r, vals)

        s0, m1, s1, m2, s2 = {}, {}, {}, {}, {}
        for r in range(-4, 12):
            s0[r] = start_row(r)
            if r - 1 >= -3:
                m1[r - 1] = euler(s0, r - 1)
            if r - 2 >= -2:
                nxt = euler(m1, r - 2)
                s1[r - 2] = [0.5 * (a + b) for a, b in zip(s0[r - 2], nxt)]
            if r - 3 >= -1:
                m2[r - 3] = euler(s1, r - 3)
            if r - 4 >= 0:
                nxt = euler(m2, r - 4)
                s2[r - 4] = [0.5 * (a + b) for a, b in zip(s1[r - 4], nxt)]
        for f in range(3):
            for t in range(2):
                for rg in range(2):
                    v = [s2[rg * 4 + j][f][:, t * 128 : (t + 1) * 128] for j in range(4)]
                    o = exchange_lanes(v, halves, evens)
                    for b in range(4):
                        pk[f, 1 + 4 * t + b, rows, rg * 128 : (rg + 1) * 128] = o[b]
        mine = pl.ds(pl.multiple_of(me * LOC + g * 8, 8), 8)
        for b in range(3):
            rh[b, mine, :] = pk[0, me + b, rows, :]
        for k in far_first:
            obs_copy(g, k, True).start()

    def field_copy(k, mine):
        d = peer(k)
        owner = me if mine else source(k)
        return pltpu.make_async_remote_copy(
            src_ref=pk.at[1:3, 1 + d, :, :],
            dst_ref=xf.at[:, pl.ds(pl.multiple_of(owner * LOC, LOC), LOC), :],
            send_sem=f_send.at[k], recv_sem=f_recv.at[k],
            device_id={"member": d}, device_id_type=MESH,
        )

    for k in far_first:
        field_copy(k, True).start()
    own = pl.ds(pl.multiple_of(me * LOC, LOC), LOC)
    for f in range(2):
        xf[f, own, :] = pk[1 + f, 1 + me, :, :]

    @pl.loop(0, 8)
    def _(g):
        for k in range(1, NM):
            obs_copy(g, k, False).wait_recv()

    for b in range(3):
        co[b, 2:3, :] = jnp.sum(rh[b], axis=0, keepdims=True) * (1.0 / ENS)
    c_at = iota((1, CELLS), 1)
    row_of = (c_at >> 5).astype(F32)
    col_of = (c_at & 31).astype(F32)

    def gram_copy(a, n):
        return pltpu.make_async_remote_copy(
            src_ref=gs.at[a, n], dst_ref=gr.at[a, n],
            send_sem=g_send.at[a, n], recv_sem=g_recv.at[a, n],
            device_id={"lat": north if a == 0 else south}, device_id_type=MESH,
        )

    def drive_copy(a):
        return pltpu.make_async_remote_copy(
            src_ref=ds_.at[a], dst_ref=dr.at[a],
            send_sem=g_send.at[a, 3], recv_sem=g_recv.at[a, 3],
            device_id={"lat": north if a == 0 else south}, device_id_type=MESH,
        )

    drive0 = None
    for a, offset in ((0, -1), (1, 1), (2, 0)):
        inside = {-1: in_north, 1: in_south, 0: 1.0}[offset]
        pushes = []
        for b in range(3):
            up = ((row_of - offset * ROWS) - 0.5 * (ROWS - 1)) / ROWS
            east = ((col_of + (b - 1) * 32) - 0.5 * 31) / 32
            t_root = jnp.exp(-0.25 * (up * up + east * east)) * inside
            s_w = t_root * co[b, 0:1, :]
            y_bar = co[b, 2:3, :]
            pushes.append(t_root * (co[b, 1:2, :] - y_bar * co[b, 0:1, :]))

            @pl.loop(0, ENS // 64)
            def _(n):
                r = pl.ds(pl.multiple_of(n * 64, 64), 64)
                s_h, s_l = split((rh[b, r, :] - y_bar) * s_w)
                sh[r, b * CELLS : (b + 1) * CELLS] = s_h
                sl[r, b * CELLS : (b + 1) * CELLS] = s_l

        drive = row_times(jnp.concatenate(pushes, axis=1), sh[...], sl[...], NT)
        if a < 2:
            ds_[a] = jnp.broadcast_to(drive, (8, ENS))
        else:
            drive0 = drive
        for n, (i, j) in enumerate(BLOCKS):
            ri, rj = slice(i * 256, (i + 1) * 256), slice(j * 256, (j + 1) * 256)
            acc = dot(sh[ri, :], sh[rj, :], NT) + dot(sh[ri, :], sl[rj, :], NT)
            acc = acc + dot(sl[ri, :], sh[rj, :], NT)
            if a < 2:
                gs[a, n] = acc
                gram_copy(a, n).start()
            else:
                g0[n] = acc
        if a < 2:
            drive_copy(a).start()

    for a in range(2):
        for n in range(3):
            gram_copy(a, n).wait_recv()
        drive_copy(a).wait_recv()
    drive = drive0 + dr[0, 0:1, :] + dr[1, 0:1, :]

    squares = jnp.zeros((8, 256), F32)
    for n, (i, j) in enumerate(BLOCKS):
        for part in range(4):
            r = slice(part * 64, (part + 1) * 64)
            tot = g0[n, r, :] + gr[0, n, r, :] + gr[1, n, r, :]
            if i == j:
                tot = tot + jnp.where(iota((64, 256), 0) + part * 64 == iota((64, 256), 1), ENS - 1.0, 0.0)
            g0[n, r, :] = tot
            sq = jnp.sum((tot * tot).reshape(8, 8, 256), axis=0)
            squares = squares + (sq if i == j else 2.0 * sq)
    fro = jnp.sqrt(jnp.sum(squares, axis=(0, 1), keepdims=True))
    inv_fro = 1.0 / fro

    def span(i):
        return slice(i * 256, (i + 1) * 256)

    def put(h, l, i, j, v):
        v_h, v_l = split(v)
        h[span(i), span(j)] = v_h
        l[span(i), span(j)] = v_l
        if i < j:
            h[span(j), span(i)] = v_h.T
            l[span(j), span(i)] = v_l.T

    def mul(a_h, a_l, b_h, b_l, i, j):
        acc = dot(a_h[span(i), :], b_h[:, span(j)]) + dot(a_h[span(i), :], b_l[:, span(j)])
        return acc + dot(a_l[span(i), :], b_h[:, span(j)])

    def eye(i, j, scale):
        if i != j:
            return 0.0
        return jnp.where(iota((256, 256), 0) == iota((256, 256), 1), scale, 0.0)

    def square(a_h, a_l):
        for i, j in BLOCKS:
            m = mf[span(i), span(j)]
            m2 = mul(a_h, a_l, a_h, a_l, i, j)
            put(bh, bl, i, j, m2)
            put(qh, ql, i, j, 0.0625 * m2 - 0.5625 * m)
            rf[span(i), span(j)] = (1.6875 * m2 - 2.4375 * m) + eye(i, j, 2.25)

    def pair_factor(to_h, to_l):
        for i, j in BLOCKS:
            put(to_h, to_l, i, j, rf[span(i), span(j)] + mul(bh, bl, qh, ql, i, j))

    def times(to_h, to_l, a_h, a_l, b_h, b_l):
        new = [mul(a_h, a_l, b_h, b_l, i, j) for i, j in BLOCKS]
        for (i, j), v in zip(BLOCKS, new):
            put(to_h, to_l, i, j, v)

    for n, (i, j) in enumerate(BLOCKS):
        scaled = g0[n] * inv_fro
        mf[span(i), span(j)] = scaled
        put(yh, yl, i, j, scaled)
    square(yh, yl)
    pair_factor(zh, zl)
    times(yh, yl, yh, yl, zh, zl)

    def step():
        for i, j in BLOCKS:
            m = mul(zh, zl, yh, yl, i, j)
            mf[span(i), span(j)] = m
            put(mh, ml, i, j, m)
        square(mh, ml)
        pair_factor(gh, gl)

    @pl.loop(0, 4)
    def _(n):
        step()
        times(yh, yl, yh, yl, gh, gl)
        times(zh, zl, gh, gl, zh, zl)

    step()
    times(zh, zl, gh, gl, zh, zl)

    for k in range(1, NM):
        field_copy(k, False).wait_recv()
    bars = []
    for f in range(3):
        ref = rh.at[1] if f == 0 else xf.at[f - 1]
        bar = co[1, 2:3, :] if f == 0 else jnp.sum(ref[...], axis=0, keepdims=True) * (1.0 / ENS)
        bars.append(bar)

        @pl.loop(0, ENS // 64)
        def _(n):
            r = pl.ds(pl.multiple_of(n * 64, 64), 64)
            x_h, x_l = split(ref[r, :] - bar)
            xh[r, f * CELLS : (f + 1) * CELLS] = x_h
            xl[r, f * CELLS : (f + 1) * CELLS] = x_l

    mean_weight = row_times(row_times(drive, zh[...], zl[...]), zh[...], zl[...]) * inv_fro
    bias = jnp.concatenate(bars, axis=1) + row_times(mean_weight, xh[...], xl[...])
    scale = math.sqrt(ENS - 1.0) / jnp.sqrt(fro)

    def analysis_copy(k, mine):
        d = peer(k)
        owner = me if mine else source(k)
        return pltpu.make_async_remote_copy(
            src_ref=ao.at[:, pl.ds(pl.multiple_of(d * LOC, LOC), LOC), :],
            dst_ref=ro.at[:, owner, :, :],
            send_sem=a_send.at[k], recv_sem=a_recv.at[k],
            device_id={"member": d}, device_id_type=MESH,
        )

    def analysed(d):
        r = pl.ds(pl.multiple_of(d * LOC, LOC), LOC)
        both = dot(jnp.concatenate([zh[r, :], zl[r, :]], axis=0), xh[...])
        acc = both[0:LOC] + both[LOC : 2 * LOC] + dot(zh[r, :], xl[...])
        return acc * scale + bias

    for k in far_first:
        d = peer(k)
        r = pl.ds(pl.multiple_of(d * LOC, LOC), LOC)
        res = analysed(d)
        for f in range(3):
            ao[f, r, :] = res[:, f * CELLS : (f + 1) * CELLS]
        analysis_copy(k, True).start()
    res = analysed(me)
    for f in range(3):
        ro[f, me, :, :] = res[:, f * CELLS : (f + 1) * CELLS]
    for k in range(1, NM):
        analysis_copy(k, False).wait_recv()

    @pl.loop(0, 8)
    def _(g):
        rows = pl.ds(pl.multiple_of(g * 8, 8), 8)
        for f in range(3):
            for t in range(2):
                for rg in range(2):
                    v = [ro[f, 4 * t + b, rows, rg * 128 : (rg + 1) * 128] for b in range(4)]
                    o = exchange_lanes(v, halves, evens)
                    for j in range(4):
                        out[f, rg * 4 + j, rows, t * 128 : (t + 1) * 128] = o[j]

    @pl.loop(0, 8)
    def _(g):
        halo(0, g).wait_send()
        halo(1, g).wait_send()
        for k in range(1, NM):
            obs_copy(g, k, True).wait_send()

    for k in range(1, NM):
        field_copy(k, True).wait_send()
        analysis_copy(k, True).wait_send()
    for a in range(2):
        for n in range(3):
            gram_copy(a, n).wait_send()
        drive_copy(a).wait_send()


def body(ensemble_state, obs_cell, obs_value, obs_prec):
    by_row = ensemble_state.transpose(0, 2, 1, 3)
    vmem = pl.BlockSpec(memory_space=pltpu.VMEM)
    half = pltpu.VMEM((ENS, ENS), BF16)
    full = pltpu.VMEM((ENS, ENS), F32)
    dma = pltpu.SemaphoreType.DMA
    analysed = pl.pallas_call(
        kernel,
        out_shape=jax.ShapeDtypeStruct((3, ROWS, LOC, LON), F32),
        in_specs=[vmem] * 4,
        out_specs=vmem,
        scratch_shapes=[
            pltpu.VMEM((3, 4, LOC, LON), F32),
            pltpu.VMEM((3, 4, LOC, LON), F32),
            pltpu.VMEM((3, 10, LOC, CELLS), F32),
            pltpu.VMEM((3, ENS, CELLS), F32),
            pltpu.VMEM((2, ENS, CELLS), F32),
            pltpu.VMEM((ENS, 768), BF16),
            pltpu.VMEM((ENS, 768), BF16),
            pltpu.VMEM((3, 256, 256), F32),
            pltpu.VMEM((2, 3, 256, 256), F32),
            pltpu.VMEM((2, 3, 256, 256), F32),
            pltpu.VMEM((2, 8, ENS), F32),
            pltpu.VMEM((2, 8, ENS), F32),
            pltpu.VMEM((3, 8, CELLS), F32),
        ]
        + [half] * 12
        + [full] * 2
        + [
            pltpu.VMEM((ENS, 768), BF16),
            pltpu.VMEM((ENS, 768), BF16),
            pltpu.VMEM((3, ENS, CELLS), F32),
            pltpu.VMEM((3, NM, LOC, CELLS), F32),
            dma((2, 8)),
            dma((2, 8)),
            dma((8, 8)),
            dma((8, 8)),
            dma((8,)),
            dma((8,)),
            dma((2, 4)),
            dma((2, 4)),
            dma((8,)),
            dma((8,)),
        ],
        compiler_params=pltpu.CompilerParams(
            collective_id=0, has_side_effects=True, vmem_limit_bytes=60 << 20
        ),
        name="letkf_cycle",
    )(by_row, obs_cell, obs_value, obs_prec)
    return analysed.transpose(0, 2, 1, 3)


def solution(mesh):
    in_specs = (P(None, "member", "lat", None), P(), P(), P())
    out_specs = P(None, "member", "lat", None)
    return jax.shard_map(body, mesh=mesh, in_specs=in_specs, out_specs=out_specs, check_vma=False)
```

```python
import math

import jax
import jax.numpy as jnp
from jax import lax
from jax.experimental import pallas as pl
from jax.experimental.pallas import tpu as pltpu
from jax.sharding import PartitionSpec as P

MESH = pl.DeviceIdType.MESH
F32 = jnp.float32
BF16 = jnp.bfloat16
NM = 8
NL = 16
ENS = 512
LOC = 64
ROWS = 8
LON = 256
CELLS = 256
DT = 0.3
NN = (((1,), (0,)), ((), ()))
NT = (((1,), (1,)), ((), ()))
BLOCKS = ((0, 0), (0, 1), (1, 1))


def dot(a, b, dims=NN):
    return lax.dot_general(a, b, dims, preferred_element_type=F32)


def split(v):
    high = v.astype(BF16)
    low = (v - high.astype(F32)).astype(BF16)
    return high, low


def iota(shape, dim):
    return lax.broadcasted_iota(jnp.int32, shape, dim)


def exchange_lanes(v, halves, evens):
    a0 = jnp.where(halves, v[0], pltpu.roll(v[2], 64, 1))
    a2 = jnp.where(halves, pltpu.roll(v[0], 64, 1), v[2])
    a1 = jnp.where(halves, v[1], pltpu.roll(v[3], 64, 1))
    a3 = jnp.where(halves, pltpu.roll(v[1], 64, 1), v[3])
    o0 = jnp.where(evens, a0, pltpu.roll(a1, 32, 1))
    o1 = jnp.where(evens, pltpu.roll(a0, 96, 1), a1)
    o2 = jnp.where(evens, a2, pltpu.roll(a3, 32, 1))
    o3 = jnp.where(evens, pltpu.roll(a2, 96, 1), a3)
    return [o0, o1, o2, o3]


def row_times(row, mat_h, mat_l, dims=NN):
    high = row.astype(BF16).astype(F32)
    lhs = jnp.concatenate([high, row - high, jnp.zeros((6, row.shape[1]), F32)], axis=0)
    lhs = lhs.astype(BF16)
    first = dot(lhs, mat_h, dims)
    second = dot(lhs, mat_l, dims)
    return first[0:1] + first[1:2] + second[0:1]


def kernel(
    x_in, cell_in, val_in, prec_in, ro, bo,
    xn, cell, val, prec, xs, ht, hb, pk, rh, xf, sh, sl, s2h, s2l, g0, gs, gr, ds_, dr, co,
    yh, yl, zh, zl, mh, ml, bh, bl, qh, ql, gh, gl, mf, rf, xh, xl, ao, bs,
    in_sem, h_send, h_recv, o_send, o_recv, f_send, f_recv, g_send, g_recv, a_send, a_recv,
):
    me = lax.axis_index("member")
    lat = lax.axis_index("lat")
    south = lax.rem(lat + 1, NL)
    north = lax.rem(lat + NL - 1, NL)

    def peer(k):
        return lax.rem(me + k, NM)

    def source(k):
        return lax.rem(me + NM - k, NM)

    def state_in(g):
        rows = pl.ds(pl.multiple_of(g * 8, 8), 8)
        return pltpu.make_async_copy(x_in.at[:, rows], xn.at[:, rows], in_sem.at[g])

    obs_in = [
        pltpu.make_async_copy(a.at[lat], b, in_sem.at[8 + i])
        for i, (a, b) in enumerate(((cell_in, cell), (val_in, val), (prec_in, prec)))
    ]
    for g in range(8):
        state_in(g).start()
    for c in obs_in:
        c.start()
    barrier = pltpu.get_barrier_semaphore()
    for k in range(1, NM):
        pl.semaphore_signal(barrier, inc=1, device_id={"member": peer(k)}, device_id_type=MESH)
    for there in (north, south):
        pl.semaphore_signal(barrier, inc=1, device_id={"lat": there}, device_id_type=MESH)

    with jax.named_scope("load"):

        @pl.loop(0, 8)
        def _(g):
            state_in(g).wait()
            rows = pl.ds(pl.multiple_of(g * 8, 8), 8)
            for f in range(3):
                for r in range(ROWS):
                    xs[f, r, rows, :] = xn[f, rows, r, :]

    with jax.named_scope("barrier"):
        pl.semaphore_wait(barrier, NM + 1)

    def halo(side, g):
        rows = pl.ds(pl.multiple_of(g * 8, 8), 8)
        src = xs.at[:, 0:4, rows, :] if side == 0 else xs.at[:, 4:8, rows, :]
        dst = (hb if side == 0 else ht).at[:, :, rows, :]
        return pltpu.make_async_remote_copy(
            src_ref=src, dst_ref=dst, send_sem=h_send.at[side, g], recv_sem=h_recv.at[side, g],
            device_id={"lat": north if side == 0 else south}, device_id_type=MESH,
        )

    @pl.loop(0, 8)
    def _(g):
        halo(0, g).start()
        halo(1, g).start()

    for c in obs_in:
        c.wait()
    cells_at = iota((CELLS, CELLS), 0)
    for b in range(3):
        q = me + (b - 1)
        q_in = jnp.clip(q, 0, NM - 1)
        there = ((q >= 0) & (q < NM)).astype(jnp.int32).astype(F32)
        c_row = cell[pl.ds(q_in, 1), :]
        p_row = prec[pl.ds(q_in, 1), :] * there
        v_row = val[pl.ds(q_in, 1), :] * p_row
        parts = []
        for r in (p_row, v_row):
            one = r.astype(BF16).astype(F32)
            two = (r - one).astype(BF16).astype(F32)
            parts += [one, two, r - one - two]
        lhs = jnp.concatenate(parts + [jnp.zeros((2, CELLS), F32)], axis=0).astype(BF16)
        hot = jnp.where(cells_at == c_row, 1.0, 0.0).astype(BF16)
        sums = dot(lhs, hot, NT)
        p_sum = sums[0:1] + sums[1:2] + sums[2:3]
        v_sum = sums[3:4] + sums[4:5] + sums[5:6]
        root = jnp.sqrt(p_sum)
        co[b, 0:1, :] = root
        co[b, 1:2, :] = jnp.where(p_sum > 0.0, v_sum / jnp.where(p_sum > 0.0, root, 1.0), 0.0)

    lane = iota((8, LON), 1)
    west_edge = lane == 0
    east_edge = lane == LON - 1
    lane1 = iota((8, 128), 1)
    halves = lane1 < 64
    evens = (lane1 & 32) == 0
    in_north = jnp.minimum(lat, 1).astype(F32)
    in_south = jnp.minimum(NL - 1 - lat, 1).astype(F32)

    def mask_row(r, state):
        if r < 0:
            return [s * in_north for s in state]
        if r >= ROWS:
            return [s * in_south for s in state]
        return state

    def slope(q):
        east = jnp.where(east_edge, 0.0, pltpu.roll(q, LON - 1, 1))
        west = jnp.where(west_edge, 0.0, pltpu.roll(q, 1, 1))
        return east - west

    half = 0.5 * DT

    def euler(states, r):
        h, u, v = states[r]
        above, below = states[r - 1], states[r + 1]
        spin = DT * (0.5 + ((lat * ROWS + r).astype(F32) * (1.0 / (NL * ROWS)) - 0.5))
        nh = h - half * (slope(u) + (below[2] - above[2]))
        nu = u - half * slope(h) + spin * v
        nv = v - half * (below[0] - above[0]) - spin * u
        return mask_row(r, [nh, nu, nv])

    pk[0, 0, :, :] = jnp.zeros((LOC, CELLS), F32)

    @pl.when(me == NM - 1)
    def _():
        rh[2] = jnp.zeros((ENS, CELLS), F32)

    def obs_copy(g, k, mine):
        d = peer(k)
        src = pk.at[0, pl.ds(d, 2), pl.ds(pl.multiple_of(g * 8, 8), 8), :]
        owner = me if mine else source(k)
        dst = rh.at[0:2, pl.ds(pl.multiple_of(owner * LOC + g * 8, 8), 8), :]
        return pltpu.make_async_remote_copy(
            src_ref=src, dst_ref=dst, send_sem=o_send.at[g, k], recv_sem=o_recv.at[g, k],
            device_id={"member": d}, device_id_type=MESH,
        )

    def east_copy(k, mine):
        d = peer(k)
        owner = me if mine else source(k)
        return pltpu.make_async_remote_copy(
            src_ref=pk.at[0, d + 2, :, :],
            dst_ref=rh.at[2, pl.ds(pl.multiple_of(owner * LOC, LOC), LOC), :],
            send_sem=o_send.at[8, k], recv_sem=o_recv.at[8, k],
            device_id={"member": d}, device_id_type=MESH,
        )

    far_first = (4, 2, 6, 3, 5, 1, 7)

    @pl.loop(0, 8)
    def _(g):
        halo(0, g).wait_recv()
        halo(1, g).wait_recv()
        rows = pl.ds(pl.multiple_of(g * 8, 8), 8)

        def start_row(r):
            if r < 0:
                vals = [ht[f, r + 4, rows, :] for f in range(3)]
            elif r >= ROWS:
                vals = [hb[f, r - ROWS, rows, :] for f in range(3)]
            else:
                vals = [xs[f, r, rows, :] for f in range(3)]
            return mask_row(r, vals)

        s0, m1, s1, m2, s2 = {}, {}, {}, {}, {}
        for r in range(-4, 12):
            s0[r] = start_row(r)
            if r - 1 >= -3:
                m1[r - 1] = euler(s0, r - 1)
            if r - 2 >= -2:
                nxt = euler(m1, r - 2)
                s1[r - 2] = [0.5 * (a + b) for a, b in zip(s0[r - 2], nxt)]
            if r - 3 >= -1:
                m2[r - 3] = euler(s1, r - 3)
            if r - 4 >= 0:
                nxt = euler(m2, r - 4)
                s2[r - 4] = [0.5 * (a + b) for a, b in zip(s1[r - 4], nxt)]
        for f in range(3):
            for t in range(2):
                for rg in range(2):
                    v = [s2[rg * 4 + j][f][:, t * 128 : (t + 1) * 128] for j in range(4)]
                    o = exchange_lanes(v, halves, evens)
                    for b in range(4):
                        pk[f, 1 + 4 * t + b, rows, rg * 128 : (rg + 1) * 128] = o[b]
        mine = pl.ds(pl.multiple_of(me * LOC + g * 8, 8), 8)
        for b in range(2):
            rh[b, mine, :] = pk[0, me + b, rows, :]
        for k in far_first:
            obs_copy(g, k, True).start()

    def field_copy(k, mine):
        d = peer(k)
        owner = me if mine else source(k)
        return pltpu.make_async_remote_copy(
            src_ref=pk.at[1:3, 1 + d, :, :],
            dst_ref=xf.at[:, pl.ds(pl.multiple_of(owner * LOC, LOC), LOC), :],
            send_sem=f_send.at[k], recv_sem=f_recv.at[k],
            device_id={"member": d}, device_id_type=MESH,
        )

    for k in far_first:

        @pl.when(peer(k) < NM - 1)
        def _():
            east_copy(k, True).start()

    for k in far_first:
        field_copy(k, True).start()
    own = pl.ds(pl.multiple_of(me * LOC, LOC), LOC)
    for f in range(2):
        xf[f, own, :] = pk[1 + f, 1 + me, :, :]

    @pl.when(me < NM - 1)
    def _():
        rh[2, own, :] = pk[0, me + 2, :, :]

    with jax.named_scope("obs01"):

        @pl.loop(0, 8)
        def _(g):
            for k in range(1, NM):
                obs_copy(g, k, False).wait_recv()

    odd = lax.rem(lat, 2)
    first_peer = lax.rem(lat + NL - 1 + 2 * odd, NL)
    second_peer = lax.rem(lat + NL + 1 - 2 * odd, NL)
    odd_f = odd.astype(F32)
    shifts = (2.0 * odd_f - 1.0, 1.0 - 2.0 * odd_f, 0.0)
    insides = (
        in_north * (1.0 - odd_f) + in_south * odd_f,
        in_south * (1.0 - odd_f) + in_north * odd_f,
        1.0,
    )
    c_at = iota((1, CELLS), 1)
    row_of = (c_at >> 5).astype(F32)
    col_of = (c_at & 31).astype(F32)

    def remote_gram(a, src, dst, n):
        return pltpu.make_async_remote_copy(
            src_ref=src, dst_ref=dst, send_sem=g_send.at[a, n], recv_sem=g_recv.at[a, n],
            device_id={"lat": first_peer if a == 0 else second_peer}, device_id_type=MESH,
        )

    low, top = slice(128, 256), slice(0, 128)

    def gram_copies(a, n):
        if n == 1:
            return [remote_gram(a, gs.at[a, 1], gr.at[a, 1], 2)]
        at = 0 if n == 0 else 3
        return [
            remote_gram(a, gs.at[a, n, top, :], gr.at[a, n, top, :], at),
            remote_gram(a, gs.at[a, n, low, low], gr.at[a, n, low, low], at + 1),
        ]

    def drive_copy(a):
        return remote_gram(a, ds_.at[a], dr.at[a], 5)

    def member_mean(b):
        co[b, 2:3, :] = jnp.sum(rh[b], axis=0, keepdims=True) * (1.0 / ENS)

    def weigh(a, b, to_h, to_l, at):
        up = ((row_of - shifts[a] * ROWS) - 0.5 * (ROWS - 1)) / ROWS
        east = ((col_of + (b - 1) * 32) - 0.5 * 31) / 32
        t_root = jnp.exp(-0.25 * (up * up + east * east)) * insides[a]
        s_w = t_root * co[b, 0:1, :]
        y_bar = co[b, 2:3, :]

        @pl.loop(0, ENS // 64)
        def _(n):
            r = pl.ds(pl.multiple_of(n * 64, 64), 64)
            s_h, s_l = split((rh[b, r, :] - y_bar) * s_w)
            to_h[r, at : at + CELLS] = s_h
            to_l[r, at : at + CELLS] = s_l

        return t_root * (co[b, 1:2, :] - y_bar * co[b, 0:1, :])

    def products(h, l, i, j):
        ri, rj = slice(i * 256, (i + 1) * 256), slice(j * 256, (j + 1) * 256)
        acc = dot(h[ri, :], h[rj, :], NT) + dot(h[ri, :], l[rj, :], NT)
        return acc + dot(l[ri, :], h[rj, :], NT)

    for b in range(2):
        member_mean(b)
    drives = []
    with jax.named_scope("gram01"):
        for a in range(3):
            push = [weigh(a, b, sh, sl, b * CELLS) for b in range(2)]
            drives.append(row_times(jnp.concatenate(push, axis=1), sh[...], sl[...], NT))
            for n, (i, j) in enumerate(BLOCKS):
                if a < 2:
                    gs[a, n] = products(sh, sl, i, j)
                else:
                    g0[n] = products(sh, sl, i, j)

    with jax.named_scope("obs2"):

        @pl.when(me < NM - 1)
        def _():
            for k in range(1, NM):
                east_copy(k, False).wait_recv()

    member_mean(2)
    with jax.named_scope("gram2"):
        for a in range(3):
            push = weigh(a, 2, s2h, s2l, 0)
            for n, (i, j) in enumerate(BLOCKS):
                if a < 2:
                    gs[a, n] = gs[a, n] + products(s2h, s2l, i, j)
                    for c in gram_copies(a, n):
                        c.start()
                else:
                    g0[n] = g0[n] + products(s2h, s2l, i, j)
            drives[a] = drives[a] + row_times(push, s2h[...], s2l[...], NT)
            if a < 2:
                ds_[a] = jnp.broadcast_to(drives[a], (8, ENS))
                drive_copy(a).start()

    with jax.named_scope("gwait"):
        for a in range(2):
            for n in range(3):
                for c in gram_copies(a, n):
                    c.wait_recv()
            drive_copy(a).wait_recv()
    drive = drives[2] + dr[0, 0:1, :] + dr[1, 0:1, :]

    squares = jnp.zeros((8, 128), F32)
    for n, (i, j) in enumerate(BLOCKS):
        for part in range(4):
            if i == j and part >= 2:
                lanes = ((part * 64, 128),)
            else:
                lanes = ((0, 0), (0, 128))
            for _unused, c0 in lanes:
                r, c = slice(part * 64, (part + 1) * 64), slice(c0, c0 + 128)
                tot = g0[n, r, c] + gr[0, n, r, c] + gr[1, n, r, c]
                if i == j:
                    on = iota((64, 128), 0) + part * 64 == iota((64, 128), 1) + c0
                    tot = tot + jnp.where(on, ENS - 1.0, 0.0)
                g0[n, r, c] = tot
                sq = jnp.sum((tot * tot).reshape(8, 8, 128), axis=0)
                twice = i != j or (part < 2 and c0 == 128)
                squares = squares + (2.0 * sq if twice else sq)
        if i == j:
            g0[n, low, top] = g0[n, top, low].T
    fro = jnp.sqrt(jnp.sum(squares, axis=(0, 1), keepdims=True))
    inv_fro = 1.0 / fro

    def span(i):
        return slice(i * 256, (i + 1) * 256)

    def put(h, l, i, j, v):
        v_h, v_l = split(v)
        h[span(i), span(j)] = v_h
        l[span(i), span(j)] = v_l
        if i < j:
            h[span(j), span(i)] = v_h.T
            l[span(j), span(i)] = v_l.T

    def mul(a_h, a_l, b_h, b_l, i, j):
        acc = dot(a_h[span(i), :], b_h[:, span(j)]) + dot(a_h[span(i), :], b_l[:, span(j)])
        return acc + dot(a_l[span(i), :], b_h[:, span(j)])

    def eye(i, j, scale):
        if i != j:
            return 0.0
        return jnp.where(iota((256, 256), 0) == iota((256, 256), 1), scale, 0.0)

    def square(a_h, a_l):
        for i, j in BLOCKS:
            m = mf[span(i), span(j)]
            m2 = mul(a_h, a_l, a_h, a_l, i, j)
            put(bh, bl, i, j, m2)
            put(qh, ql, i, j, 0.0625 * m2 - 0.5625 * m)
            rf[span(i), span(j)] = (1.6875 * m2 - 2.4375 * m) + eye(i, j, 2.25)

    def pair_factor(to_h, to_l):
        for i, j in BLOCKS:
            put(to_h, to_l, i, j, rf[span(i), span(j)] + mul(bh, bl, qh, ql, i, j))

    def times(to_h, to_l, a_h, a_l, b_h, b_l):
        new = [mul(a_h, a_l, b_h, b_l, i, j) for i, j in BLOCKS]
        for (i, j), v in zip(BLOCKS, new):
            put(to_h, to_l, i, j, v)

    def take_states(f):
        ref = rh.at[1] if f == 0 else xf.at[f - 1]
        if f == 0:
            bar = co[1, 2:3, :]
        else:
            bar = jnp.sum(ref[...], axis=0, keepdims=True) * (1.0 / ENS)
        bs[0:1, f * CELLS : (f + 1) * CELLS] = bar

        @pl.loop(0, ENS // 64)
        def _(n):
            r = pl.ds(pl.multiple_of(n * 64, 64), 64)
            x_h, x_l = split(ref[r, :] - bar)
            xh[r, f * CELLS : (f + 1) * CELLS] = x_h
            xl[r, f * CELLS : (f + 1) * CELLS] = x_l

    for n, (i, j) in enumerate(BLOCKS):
        scaled = g0[n] * inv_fro
        mf[span(i), span(j)] = scaled
        put(yh, yl, i, j, scaled)
    square(yh, yl)
    pair_factor(zh, zl)
    times(yh, yl, yh, yl, zh, zl)

    def step():
        for i, j in BLOCKS:
            m = mul(zh, zl, yh, yl, i, j)
            mf[span(i), span(j)] = m
            put(mh, ml, i, j, m)
        square(mh, ml)
        pair_factor(gh, gl)

    with jax.named_scope("ns"):

        @pl.loop(0, 4)
        def _(n):
            step()
            times(yh, yl, yh, yl, gh, gl)
            times(zh, zl, gh, gl, zh, zl)

    with jax.named_scope("fields"):
        for k in range(1, NM):
            field_copy(k, False).wait_recv()
    with jax.named_scope("states"):
        for f in range(3):
            take_states(f)

    with jax.named_scope("ns5"):
        step()
        times(zh, zl, gh, gl, zh, zl)
    scale = math.sqrt(ENS - 1.0) / jnp.sqrt(fro)

    def analysis_copy(k, mine):
        d = peer(k)
        owner = me if mine else source(k)
        return pltpu.make_async_remote_copy(
            src_ref=ao.at[:, pl.ds(pl.multiple_of(d * LOC, LOC), LOC), :],
            dst_ref=ro.at[:, owner, :, :],
            send_sem=a_send.at[0, k], recv_sem=a_recv.at[0, k],
            device_id={"member": d}, device_id_type=MESH,
        )

    def analysed(d):
        r = pl.ds(pl.multiple_of(d * LOC, LOC), LOC)
        both = dot(jnp.concatenate([zh[r, :], zl[r, :]], axis=0), xh[...])
        acc = both[0:LOC] + both[LOC : 2 * LOC] + dot(zh[r, :], xl[...])
        return acc * scale

    def bias_copy(k, mine):
        d = peer(k)
        owner = me if mine else source(k)
        return pltpu.make_async_remote_copy(
            src_ref=bs, dst_ref=bo.at[owner],
            send_sem=a_send.at[1, k], recv_sem=a_recv.at[1, k],
            device_id={"member": d}, device_id_type=MESH,
        )


    for k in far_first:
        d = peer(k)
        r = pl.ds(pl.multiple_of(d * LOC, LOC), LOC)
        res = analysed(d)
        for f in range(3):
            ao[f, r, :] = res[:, f * CELLS : (f + 1) * CELLS]
        analysis_copy(k, True).start()
    res = analysed(me)
    for f in range(3):
        ro[f, me, :, :] = res[:, f * CELLS : (f + 1) * CELLS]
    mean_weight = row_times(row_times(drive, zh[...], zl[...]), zh[...], zl[...]) * inv_fro
    bias = bs[0:1, :] + row_times(mean_weight, xh[...], xl[...])
    bs[...] = jnp.broadcast_to(bias, (8, 768))
    bo[me] = jnp.broadcast_to(bias, (8, 768))
    for k in far_first:
        bias_copy(k, True).start()
    with jax.named_scope("out"):
        for k in range(1, NM):
            analysis_copy(k, False).wait_recv()
            bias_copy(k, False).wait_recv()

    @pl.loop(0, 8)
    def _(g):
        halo(0, g).wait_send()
        halo(1, g).wait_send()
        for k in range(1, NM):
            obs_copy(g, k, True).wait_send()

    for k in range(1, NM):

        @pl.when(peer(k) < NM - 1)
        def _():
            east_copy(k, True).wait_send()

    for k in range(1, NM):
        field_copy(k, True).wait_send()
        analysis_copy(k, True).wait_send()
        bias_copy(k, True).wait_send()
    for a in range(2):
        for n in range(3):
            for c in gram_copies(a, n):
                c.wait_send()
        drive_copy(a).wait_send()


def unpack(ro, bo, out):
    lane1 = iota((8, 128), 1)
    halves = lane1 < 64
    evens = (lane1 & 32) == 0
    for f in range(3):
        for t in range(2):
            for rg in range(2):
                at = f * CELLS + rg * 128
                v = [
                    ro[f, 4 * t + b, :, rg * 128 : (rg + 1) * 128] + bo[4 * t + b, :, at : at + 128]
                    for b in range(4)
                ]
                o = exchange_lanes(v, halves, evens)
                for j in range(4):
                    out[f, :, rg * 4 + j, t * 128 : (t + 1) * 128] = o[j]


def body(ensemble_state, obs_cell, obs_value, obs_prec):
    vmem = pl.BlockSpec(memory_space=pltpu.VMEM)
    anywhere = pl.BlockSpec(memory_space=pltpu.HBM)
    half = pltpu.VMEM((ENS, ENS), BF16)
    full = pltpu.VMEM((ENS, ENS), F32)
    dma = pltpu.SemaphoreType.DMA
    received, biases = pl.pallas_call(
        kernel,
        out_shape=(
            jax.ShapeDtypeStruct((3, NM, LOC, CELLS), F32),
            jax.ShapeDtypeStruct((NM, 8, 768), F32),
        ),
        in_specs=[anywhere] * 4,
        out_specs=(vmem, vmem),
        scratch_shapes=[
            pltpu.VMEM((3, LOC, ROWS, LON), F32),
            pltpu.VMEM((8, 256), jnp.int32),
            pltpu.VMEM((8, 256), F32),
            pltpu.VMEM((8, 256), F32),
            pltpu.VMEM((3, ROWS, LOC, LON), F32),
            pltpu.VMEM((3, 4, LOC, LON), F32),
            pltpu.VMEM((3, 4, LOC, LON), F32),
            pltpu.VMEM((3, 10, LOC, CELLS), F32),
            pltpu.VMEM((3, ENS, CELLS), F32),
            pltpu.VMEM((2, ENS, CELLS), F32),
            pltpu.VMEM((ENS, 512), BF16),
            pltpu.VMEM((ENS, 512), BF16),
            pltpu.VMEM((ENS, 256), BF16),
            pltpu.VMEM((ENS, 256), BF16),
            pltpu.VMEM((3, 256, 256), F32),
            pltpu.VMEM((2, 3, 256, 256), F32),
            pltpu.VMEM((2, 3, 256, 256), F32),
            pltpu.VMEM((2, 8, ENS), F32),
            pltpu.VMEM((2, 8, ENS), F32),
            pltpu.VMEM((3, 8, CELLS), F32),
        ]
        + [half] * 12
        + [full] * 2
        + [
            pltpu.VMEM((ENS, 768), BF16),
            pltpu.VMEM((ENS, 768), BF16),
            pltpu.VMEM((3, ENS, CELLS), F32),
            pltpu.VMEM((8, 768), F32),
            dma((11,)),
            dma((2, 8)),
            dma((2, 8)),
            dma((9, 8)),
            dma((9, 8)),
            dma((8,)),
            dma((8,)),
            dma((2, 6)),
            dma((2, 6)),
            dma((2, 8)),
            dma((2, 8)),
        ],
        compiler_params=pltpu.CompilerParams(
            collective_id=0, has_side_effects=True, vmem_limit_bytes=40 << 20
        ),
        name="letkf_cycle",
    )(ensemble_state, obs_cell, obs_value, obs_prec)
    return pl.pallas_call(
        unpack,
        grid=(8,),
        out_shape=jax.ShapeDtypeStruct((3, LOC, ROWS, LON), F32),
        in_specs=[
            pl.BlockSpec((3, NM, 8, CELLS), lambda g: (0, 0, g, 0)),
            pl.BlockSpec((NM, 8, 768), lambda g: (0, 0, 0)),
        ],
        out_specs=pl.BlockSpec((3, 8, ROWS, LON), lambda g: (0, g, 0, 0)),
        compiler_params=pltpu.CompilerParams(vmem_limit_bytes=16 << 20),
        name="unpack",
    )(received, biases)


def solution(mesh):
    in_specs = (P(None, "member", "lat", None), P(), P(), P())
    out_specs = P(None, "member", "lat", None)
    return jax.shard_map(body, mesh=mesh, in_specs=in_specs, out_specs=out_specs, check_vma=False)
```

```python
import math

import jax
import jax.numpy as jnp
from jax import lax
from jax.experimental import pallas as pl
from jax.experimental.pallas import tpu as pltpu
from jax.sharding import PartitionSpec as P

MESH = pl.DeviceIdType.MESH
F32 = jnp.float32
BF16 = jnp.bfloat16
NM = 8
NL = 16
ENS = 512
LOC = 64
ROWS = 8
LON = 256
CELLS = 256
DT = 0.3
NN = (((1,), (0,)), ((), ()))
NT = (((1,), (1,)), ((), ()))
BLOCKS = ((0, 0), (0, 1), (1, 1))


def dot(a, b, dims=NN):
    return lax.dot_general(a, b, dims, preferred_element_type=F32)


def split(v):
    high = v.astype(BF16)
    low = (v - high.astype(F32)).astype(BF16)
    return high, low


def iota(shape, dim):
    return lax.broadcasted_iota(jnp.int32, shape, dim)


def exchange_lanes(v, halves, evens):
    a0 = jnp.where(halves, v[0], pltpu.roll(v[2], 64, 1))
    a2 = jnp.where(halves, pltpu.roll(v[0], 64, 1), v[2])
    a1 = jnp.where(halves, v[1], pltpu.roll(v[3], 64, 1))
    a3 = jnp.where(halves, pltpu.roll(v[1], 64, 1), v[3])
    o0 = jnp.where(evens, a0, pltpu.roll(a1, 32, 1))
    o1 = jnp.where(evens, pltpu.roll(a0, 96, 1), a1)
    o2 = jnp.where(evens, a2, pltpu.roll(a3, 32, 1))
    o3 = jnp.where(evens, pltpu.roll(a2, 96, 1), a3)
    return [o0, o1, o2, o3]


def row_times(row, mat_h, mat_l, dims=NN):
    high = row.astype(BF16).astype(F32)
    lhs = jnp.concatenate([high, row - high, jnp.zeros((6, row.shape[1]), F32)], axis=0)
    lhs = lhs.astype(BF16)
    first = dot(lhs, mat_h, dims)
    second = dot(lhs, mat_l, dims)
    return first[0:1] + first[1:2] + second[0:1]


def kernel(
    x_in, cell_in, val_in, prec_in, ro, bo,
    xn, cell, val, prec, xs, ht, hb, pk, rh, xf, sh, sl, s2h, s2l, g0, gs, gr, ds_, dr, co,
    yh, yl, zh, zl, mh, ml, bh, bl, qh, ql, gh, gl, mf, rf, xh, xl, ao, bs,
    in_sem, h_send, h_recv, o_send, o_recv, f_send, f_recv, g_send, g_recv, a_send, a_recv,
):
    me = lax.axis_index("member")
    lat = lax.axis_index("lat")
    south = lax.rem(lat + 1, NL)
    north = lax.rem(lat + NL - 1, NL)

    def peer(k):
        return lax.rem(me + k, NM)

    def source(k):
        return lax.rem(me + NM - k, NM)

    def state_in(g):
        rows = pl.ds(pl.multiple_of(g * 8, 8), 8)
        return pltpu.make_async_copy(x_in.at[:, rows], xn.at[:, rows], in_sem.at[g])

    obs_in = [
        pltpu.make_async_copy(a.at[lat], b, in_sem.at[8 + i])
        for i, (a, b) in enumerate(((cell_in, cell), (val_in, val), (prec_in, prec)))
    ]
    for g in range(8):
        state_in(g).start()
    for c in obs_in:
        c.start()
    barrier = pltpu.get_barrier_semaphore()
    for k in range(1, NM):
        pl.semaphore_signal(barrier, inc=1, device_id={"member": peer(k)}, device_id_type=MESH)
    for there in (north, south):
        pl.semaphore_signal(barrier, inc=1, device_id={"lat": there}, device_id_type=MESH)

    with jax.named_scope("load"):

        @pl.loop(0, 8)
        def _(g):
            state_in(g).wait()
            rows = pl.ds(pl.multiple_of(g * 8, 8), 8)
            for f in range(3):
                for r in range(ROWS):
                    xs[f, r, rows, :] = xn[f, rows, r, :]

    with jax.named_scope("barrier"):
        pl.semaphore_wait(barrier, NM + 1)

    def halo(side, g):
        rows = pl.ds(pl.multiple_of(g * 8, 8), 8)
        src = xs.at[:, 0:4, rows, :] if side == 0 else xs.at[:, 4:8, rows, :]
        dst = (hb if side == 0 else ht).at[:, :, rows, :]
        return pltpu.make_async_remote_copy(
            src_ref=src, dst_ref=dst, send_sem=h_send.at[side, g], recv_sem=h_recv.at[side, g],
            device_id={"lat": north if side == 0 else south}, device_id_type=MESH,
        )

    has_north, has_south = lat > 0, lat < NL - 1

    @pl.when(has_north)
    def _():
        for g in range(8):
            halo(0, g).start()

    @pl.when(has_south)
    def _():
        for g in range(8):
            halo(1, g).start()

    @pl.when(lat == 0)
    def _():
        ht[...] = jnp.zeros((3, 4, LOC, LON), F32)

    @pl.when(lat == NL - 1)
    def _():
        hb[...] = jnp.zeros((3, 4, LOC, LON), F32)

    for c in obs_in:
        c.wait()
    cells_at = iota((CELLS, CELLS), 0)
    for b in range(3):
        q = me + (b - 1)
        q_in = jnp.clip(q, 0, NM - 1)
        there = ((q >= 0) & (q < NM)).astype(jnp.int32).astype(F32)
        c_row = cell[pl.ds(q_in, 1), :]
        p_row = prec[pl.ds(q_in, 1), :] * there
        v_row = val[pl.ds(q_in, 1), :] * p_row
        parts = []
        for r in (p_row, v_row):
            one = r.astype(BF16).astype(F32)
            two = (r - one).astype(BF16).astype(F32)
            parts += [one, two, r - one - two]
        lhs = jnp.concatenate(parts + [jnp.zeros((2, CELLS), F32)], axis=0).astype(BF16)
        hot = jnp.where(cells_at == c_row, 1.0, 0.0).astype(BF16)
        sums = dot(lhs, hot, NT)
        p_sum = sums[0:1] + sums[1:2] + sums[2:3]
        v_sum = sums[3:4] + sums[4:5] + sums[5:6]
        root = jnp.sqrt(p_sum)
        co[b, 0:1, :] = root
        co[b, 1:2, :] = jnp.where(p_sum > 0.0, v_sum / jnp.where(p_sum > 0.0, root, 1.0), 0.0)

    lane = iota((8, LON), 1)
    west_edge = lane == 0
    east_edge = lane == LON - 1
    lane1 = iota((8, 128), 1)
    halves = lane1 < 64
    evens = (lane1 & 32) == 0
    in_north = jnp.minimum(lat, 1).astype(F32)
    in_south = jnp.minimum(NL - 1 - lat, 1).astype(F32)

    def mask_row(r, state):
        if r < 0:
            return [s * in_north for s in state]
        if r >= ROWS:
            return [s * in_south for s in state]
        return state

    def slope(q):
        east = jnp.where(east_edge, 0.0, pltpu.roll(q, LON - 1, 1))
        west = jnp.where(west_edge, 0.0, pltpu.roll(q, 1, 1))
        return east - west

    half = 0.5 * DT

    def euler(states, r):
        h, u, v = states[r]
        above, below = states[r - 1], states[r + 1]
        spin = DT * (0.5 + ((lat * ROWS + r).astype(F32) * (1.0 / (NL * ROWS)) - 0.5))
        nh = h - half * (slope(u) + (below[2] - above[2]))
        nu = u - half * slope(h) + spin * v
        nv = v - half * (below[0] - above[0]) - spin * u
        return mask_row(r, [nh, nu, nv])

    pk[0, 0, :, :] = jnp.zeros((LOC, CELLS), F32)

    @pl.when(me == NM - 1)
    def _():
        rh[2] = jnp.zeros((ENS, CELLS), F32)

    def obs_copy(g, k, mine):
        d = peer(k)
        src = pk.at[0, pl.ds(d, 2), pl.ds(pl.multiple_of(g * 8, 8), 8), :]
        owner = me if mine else source(k)
        dst = rh.at[0:2, pl.ds(pl.multiple_of(owner * LOC + g * 8, 8), 8), :]
        return pltpu.make_async_remote_copy(
            src_ref=src, dst_ref=dst, send_sem=o_send.at[g, k], recv_sem=o_recv.at[g, k],
            device_id={"member": d}, device_id_type=MESH,
        )

    def east_copy(k, mine):
        d = peer(k)
        owner = me if mine else source(k)
        return pltpu.make_async_remote_copy(
            src_ref=pk.at[0, d + 2, :, :],
            dst_ref=rh.at[2, pl.ds(pl.multiple_of(owner * LOC, LOC), LOC), :],
            send_sem=o_send.at[8, k], recv_sem=o_recv.at[8, k],
            device_id={"member": d}, device_id_type=MESH,
        )

    far_first = (4, 2, 6, 3, 5, 1, 7)

    @pl.loop(0, 8)
    def _(g):

        @pl.when(has_south)
        def _():
            halo(0, g).wait_recv()

        @pl.when(has_north)
        def _():
            halo(1, g).wait_recv()

        rows = pl.ds(pl.multiple_of(g * 8, 8), 8)

        def start_row(r):
            if r < 0:
                vals = [ht[f, r + 4, rows, :] for f in range(3)]
            elif r >= ROWS:
                vals = [hb[f, r - ROWS, rows, :] for f in range(3)]
            else:
                vals = [xs[f, r, rows, :] for f in range(3)]
            return vals

        s0, m1, s1, m2, s2 = {}, {}, {}, {}, {}
        for r in range(-4, 12):
            s0[r] = start_row(r)
            if r - 1 >= -3:
                m1[r - 1] = euler(s0, r - 1)
            if r - 2 >= -2:
                nxt = euler(m1, r - 2)
                s1[r - 2] = [0.5 * (a + b) for a, b in zip(s0[r - 2], nxt)]
            if r - 3 >= -1:
                m2[r - 3] = euler(s1, r - 3)
            if r - 4 >= 0:
                nxt = euler(m2, r - 4)
                s2[r - 4] = [0.5 * (a + b) for a, b in zip(s1[r - 4], nxt)]
        for f in range(3):
            for t in range(2):
                for rg in range(2):
                    v = [s2[rg * 4 + j][f][:, t * 128 : (t + 1) * 128] for j in range(4)]
                    o = exchange_lanes(v, halves, evens)
                    for b in range(4):
                        pk[f, 1 + 4 * t + b, rows, rg * 128 : (rg + 1) * 128] = o[b]
        mine = pl.ds(pl.multiple_of(me * LOC + g * 8, 8), 8)
        for b in range(2):
            rh[b, mine, :] = pk[0, me + b, rows, :]
        for k in far_first:
            obs_copy(g, k, True).start()

    def field_copy(k, mine):
        d = peer(k)
        owner = me if mine else source(k)
        return pltpu.make_async_remote_copy(
            src_ref=pk.at[1:3, 1 + d, :, :],
            dst_ref=xf.at[:, pl.ds(pl.multiple_of(owner * LOC, LOC), LOC), :],
            send_sem=f_send.at[k], recv_sem=f_recv.at[k],
            device_id={"member": d}, device_id_type=MESH,
        )

    for k in far_first:

        @pl.when(peer(k) < NM - 1)
        def _():
            east_copy(k, True).start()

    own = pl.ds(pl.multiple_of(me * LOC, LOC), LOC)
    for f in range(2):
        xf[f, own, :] = pk[1 + f, 1 + me, :, :]

    @pl.when(me < NM - 1)
    def _():
        rh[2, own, :] = pk[0, me + 2, :, :]

    with jax.named_scope("obs01"):

        @pl.loop(0, 8)
        def _(g):
            for k in range(1, NM):
                obs_copy(g, k, False).wait_recv()

    odd = lax.rem(lat, 2)
    first_peer = lax.rem(lat + NL - 1 + 2 * odd, NL)
    second_peer = lax.rem(lat + NL + 1 - 2 * odd, NL)
    odd_f = odd.astype(F32)
    shifts = (2.0 * odd_f - 1.0, 1.0 - 2.0 * odd_f, 0.0)
    insides = (
        in_north * (1.0 - odd_f) + in_south * odd_f,
        in_south * (1.0 - odd_f) + in_north * odd_f,
        1.0,
    )
    c_at = iota((1, CELLS), 1)
    row_of = (c_at >> 5).astype(F32)
    col_of = (c_at & 31).astype(F32)

    def remote_gram(a, src, dst, n):
        return pltpu.make_async_remote_copy(
            src_ref=src, dst_ref=dst, send_sem=g_send.at[a, n], recv_sem=g_recv.at[a, n],
            device_id={"lat": first_peer if a == 0 else second_peer}, device_id_type=MESH,
        )

    low, top = slice(128, 256), slice(0, 128)
    has_far = has_north & has_south

    def towards(a, act):
        if a == 0:
            pl.when(has_far)(act)
        else:
            act()

    @pl.when((lat == 0) | (lat == NL - 1))
    def _():
        gr[0] = jnp.zeros((3, 256, 256), F32)
        dr[0] = jnp.zeros((8, ENS), F32)

    def gram_copies(a, n):
        if n == 1:
            return [remote_gram(a, gs.at[a, 1], gr.at[a, 1], 2)]
        at = 0 if n == 0 else 3
        return [
            remote_gram(a, gs.at[a, n, top, :], gr.at[a, n, top, :], at),
            remote_gram(a, gs.at[a, n, low, low], gr.at[a, n, low, low], at + 1),
        ]

    def drive_copy(a):
        return remote_gram(a, ds_.at[a], dr.at[a], 5)

    def member_mean(b):
        co[b, 2:3, :] = jnp.sum(rh[b], axis=0, keepdims=True) * (1.0 / ENS)

    def weigh(a, b, to_h, to_l, at):
        up = ((row_of - shifts[a] * ROWS) - 0.5 * (ROWS - 1)) / ROWS
        east = ((col_of + (b - 1) * 32) - 0.5 * 31) / 32
        t_root = jnp.exp(-0.25 * (up * up + east * east)) * insides[a]
        s_w = t_root * co[b, 0:1, :]
        y_bar = co[b, 2:3, :]

        @pl.loop(0, ENS // 64)
        def _(n):
            r = pl.ds(pl.multiple_of(n * 64, 64), 64)
            s_h, s_l = split((rh[b, r, :] - y_bar) * s_w)
            to_h[r, at : at + CELLS] = s_h
            to_l[r, at : at + CELLS] = s_l

        return t_root * (co[b, 1:2, :] - y_bar * co[b, 0:1, :])

    def products(h, l, i, j):
        ri, rj = slice(i * 256, (i + 1) * 256), slice(j * 256, (j + 1) * 256)
        acc = dot(h[ri, :], h[rj, :], NT) + dot(h[ri, :], l[rj, :], NT)
        return acc + dot(l[ri, :], h[rj, :], NT)

    for b in range(2):
        member_mean(b)
    drives = []
    with jax.named_scope("gram01"):
        for a in range(3):
            push = [weigh(a, b, sh, sl, b * CELLS) for b in range(2)]
            drives.append(row_times(jnp.concatenate(push, axis=1), sh[...], sl[...], NT))
            for n, (i, j) in enumerate(BLOCKS):
                if a < 2:
                    gs[a, n] = products(sh, sl, i, j)
                else:
                    g0[n] = products(sh, sl, i, j)

    with jax.named_scope("obs2"):

        @pl.when(me < NM - 1)
        def _():
            for k in range(1, NM):
                east_copy(k, False).wait_recv()

    member_mean(2)
    with jax.named_scope("gram2"):
        for a in range(3):
            push = weigh(a, 2, s2h, s2l, 0)
            for n, (i, j) in enumerate(BLOCKS):
                if a < 2:
                    gs[a, n] = gs[a, n] + products(s2h, s2l, i, j)

                    def send(a=a, n=n):
                        for c in gram_copies(a, n):
                            c.start()

                    towards(a, send)
                else:
                    g0[n] = g0[n] + products(s2h, s2l, i, j)
            drives[a] = drives[a] + row_times(push, s2h[...], s2l[...], NT)
            if a < 2:
                ds_[a] = jnp.broadcast_to(drives[a], (8, ENS))
                towards(a, lambda a=a: drive_copy(a).start())
            if a == 1:
                for k in far_first:
                    field_copy(k, True).start()

    with jax.named_scope("gwait"):
        for a in range(2):

            def arrive(a=a):
                for n in range(3):
                    for c in gram_copies(a, n):
                        c.wait_recv()
                drive_copy(a).wait_recv()

            towards(a, arrive)
    drive = drives[2] + dr[0, 0:1, :] + dr[1, 0:1, :]

    squares = jnp.zeros((8, 128), F32)
    for n, (i, j) in enumerate(BLOCKS):
        for part in range(4):
            if i == j and part >= 2:
                lanes = ((part * 64, 128),)
            else:
                lanes = ((0, 0), (0, 128))
            for _unused, c0 in lanes:
                r, c = slice(part * 64, (part + 1) * 64), slice(c0, c0 + 128)
                tot = g0[n, r, c] + gr[0, n, r, c] + gr[1, n, r, c]
                if i == j:
                    on = iota((64, 128), 0) + part * 64 == iota((64, 128), 1) + c0
                    tot = tot + jnp.where(on, ENS - 1.0, 0.0)
                g0[n, r, c] = tot
                sq = jnp.sum((tot * tot).reshape(8, 8, 128), axis=0)
                twice = i != j or (part < 2 and c0 == 128)
                squares = squares + (2.0 * sq if twice else sq)
        if i == j:
            g0[n, low, top] = g0[n, top, low].T
    fro = jnp.sqrt(jnp.sum(squares, axis=(0, 1), keepdims=True))
    inv_fro = 1.0 / fro

    def span(i):
        return slice(i * 256, (i + 1) * 256)

    def put(h, l, i, j, v):
        v_h, v_l = split(v)
        h[span(i), span(j)] = v_h
        l[span(i), span(j)] = v_l
        if i < j:
            h[span(j), span(i)] = v_h.T
            l[span(j), span(i)] = v_l.T

    def mul(a_h, a_l, b_h, b_l, i, j):
        acc = dot(a_h[span(i), :], b_h[:, span(j)]) + dot(a_h[span(i), :], b_l[:, span(j)])
        return acc + dot(a_l[span(i), :], b_h[:, span(j)])

    def eye(i, j, scale):
        if i != j:
            return 0.0
        return jnp.where(iota((256, 256), 0) == iota((256, 256), 1), scale, 0.0)

    def square(a_h, a_l):
        for i, j in BLOCKS:
            m = mf[span(i), span(j)]
            m2 = mul(a_h, a_l, a_h, a_l, i, j)
            put(bh, bl, i, j, m2)
            put(qh, ql, i, j, 0.0625 * m2 - 0.5625 * m)
            rf[span(i), span(j)] = (1.6875 * m2 - 2.4375 * m) + eye(i, j, 2.25)

    def pair_factor(to_h, to_l):
        for i, j in BLOCKS:
            put(to_h, to_l, i, j, rf[span(i), span(j)] + mul(bh, bl, qh, ql, i, j))

    def times(to_h, to_l, a_h, a_l, b_h, b_l):
        new = [mul(a_h, a_l, b_h, b_l, i, j) for i, j in BLOCKS]
        for (i, j), v in zip(BLOCKS, new):
            put(to_h, to_l, i, j, v)

    def take_states(f):
        ref = rh.at[1] if f == 0 else xf.at[f - 1]
        if f == 0:
            bar = co[1, 2:3, :]
        else:
            bar = jnp.sum(ref[...], axis=0, keepdims=True) * (1.0 / ENS)
        bs[0:1, f * CELLS : (f + 1) * CELLS] = bar

        @pl.loop(0, ENS // 64)
        def _(n):
            r = pl.ds(pl.multiple_of(n * 64, 64), 64)
            x_h, x_l = split(ref[r, :] - bar)
            xh[r, f * CELLS : (f + 1) * CELLS] = x_h
            xl[r, f * CELLS : (f + 1) * CELLS] = x_l

    for n, (i, j) in enumerate(BLOCKS):
        scaled = g0[n] * inv_fro
        mf[span(i), span(j)] = scaled
        put(yh, yl, i, j, scaled)
    square(yh, yl)
    pair_factor(zh, zl)
    times(yh, yl, yh, yl, zh, zl)

    def step():
        for i, j in BLOCKS:
            m = mul(zh, zl, yh, yl, i, j)
            mf[span(i), span(j)] = m
            put(mh, ml, i, j, m)
        square(mh, ml)
        pair_factor(gh, gl)

    with jax.named_scope("ns"):

        @pl.loop(0, 4)
        def _(n):
            step()
            times(yh, yl, yh, yl, gh, gl)
            times(zh, zl, gh, gl, zh, zl)

    with jax.named_scope("fields"):
        for k in range(1, NM):
            field_copy(k, False).wait_recv()
    with jax.named_scope("states"):
        for f in range(3):
            take_states(f)

    with jax.named_scope("ns5"):
        step()
        times(zh, zl, gh, gl, zh, zl)
    scale = math.sqrt(ENS - 1.0) / jnp.sqrt(fro)

    def analysis_copy(k, mine):
        d = peer(k)
        owner = me if mine else source(k)
        return pltpu.make_async_remote_copy(
            src_ref=ao.at[:, pl.ds(pl.multiple_of(d * LOC, LOC), LOC), :],
            dst_ref=ro.at[:, owner, :, :],
            send_sem=a_send.at[0, k], recv_sem=a_recv.at[0, k],
            device_id={"member": d}, device_id_type=MESH,
        )

    def analysed(d):
        r = pl.ds(pl.multiple_of(d * LOC, LOC), LOC)
        both = dot(jnp.concatenate([zh[r, :], zl[r, :]], axis=0), xh[...])
        acc = both[0:LOC] + both[LOC : 2 * LOC] + dot(zh[r, :], xl[...])
        return acc * scale

    def bias_copy(k, mine):
        d = peer(k)
        owner = me if mine else source(k)
        return pltpu.make_async_remote_copy(
            src_ref=bs, dst_ref=bo.at[owner],
            send_sem=a_send.at[1, k], recv_sem=a_recv.at[1, k],
            device_id={"member": d}, device_id_type=MESH,
        )


    for k in far_first:
        d = peer(k)
        r = pl.ds(pl.multiple_of(d * LOC, LOC), LOC)
        res = analysed(d)
        for f in range(3):
            ao[f, r, :] = res[:, f * CELLS : (f + 1) * CELLS]
        analysis_copy(k, True).start()
    res = analysed(me)
    for f in range(3):
        ro[f, me, :, :] = res[:, f * CELLS : (f + 1) * CELLS]
    mean_weight = row_times(row_times(drive, zh[...], zl[...]), zh[...], zl[...]) * inv_fro
    bias = bs[0:1, :] + row_times(mean_weight, xh[...], xl[...])
    bs[...] = jnp.broadcast_to(bias, (8, 768))
    bo[me] = jnp.broadcast_to(bias, (8, 768))
    for k in far_first:
        bias_copy(k, True).start()
    with jax.named_scope("out"):
        for k in range(1, NM):
            analysis_copy(k, False).wait_recv()
            bias_copy(k, False).wait_recv()

    @pl.loop(0, 8)
    def _(g):

        @pl.when(has_north)
        def _():
            halo(0, g).wait_send()

        @pl.when(has_south)
        def _():
            halo(1, g).wait_send()

        for k in range(1, NM):
            obs_copy(g, k, True).wait_send()

    for k in range(1, NM):

        @pl.when(peer(k) < NM - 1)
        def _():
            east_copy(k, True).wait_send()

    for k in range(1, NM):
        field_copy(k, True).wait_send()
        analysis_copy(k, True).wait_send()
        bias_copy(k, True).wait_send()
    for a in range(2):

        def left(a=a):
            for n in range(3):
                for c in gram_copies(a, n):
                    c.wait_send()
            drive_copy(a).wait_send()

        towards(a, left)


def unpack(ro, bo, out, held, sem):
    lane1 = iota((8, 128), 1)
    halves = lane1 < 64
    evens = (lane1 & 32) == 0

    def leave(g):
        rows = pl.ds(pl.multiple_of(g * 8, 8), 8)
        return pltpu.make_async_copy(held.at[:, rows], out.at[:, rows], sem.at[g])

    @pl.loop(0, 8)
    def _(g):
        rows = pl.ds(pl.multiple_of(g * 8, 8), 8)
        for f in range(3):
            for t in range(2):
                for rg in range(2):
                    at = f * CELLS + rg * 128
                    v = [
                        ro[f, 4 * t + b, rows, rg * 128 : (rg + 1) * 128]
                        + bo[4 * t + b, :, at : at + 128]
                        for b in range(4)
                    ]
                    o = exchange_lanes(v, halves, evens)
                    for j in range(4):
                        held[f, rows, rg * 4 + j, t * 128 : (t + 1) * 128] = o[j]
        leave(g).start()

    for g in range(8):
        leave(g).wait()


def body(ensemble_state, obs_cell, obs_value, obs_prec):
    vmem = pl.BlockSpec(memory_space=pltpu.VMEM)
    anywhere = pl.BlockSpec(memory_space=pltpu.HBM)
    half = pltpu.VMEM((ENS, ENS), BF16)
    full = pltpu.VMEM((ENS, ENS), F32)
    dma = pltpu.SemaphoreType.DMA
    received, biases = pl.pallas_call(
        kernel,
        out_shape=(
            jax.ShapeDtypeStruct((3, NM, LOC, CELLS), F32),
            jax.ShapeDtypeStruct((NM, 8, 768), F32),
        ),
        in_specs=[anywhere] * 4,
        out_specs=(vmem, vmem),
        scratch_shapes=[
            pltpu.VMEM((3, LOC, ROWS, LON), F32),
            pltpu.VMEM((8, 256), jnp.int32),
            pltpu.VMEM((8, 256), F32),
            pltpu.VMEM((8, 256), F32),
            pltpu.VMEM((3, ROWS, LOC, LON), F32),
            pltpu.VMEM((3, 4, LOC, LON), F32),
            pltpu.VMEM((3, 4, LOC, LON), F32),
            pltpu.VMEM((3, 10, LOC, CELLS), F32),
            pltpu.VMEM((3, ENS, CELLS), F32),
            pltpu.VMEM((2, ENS, CELLS), F32),
            pltpu.VMEM((ENS, 512), BF16),
            pltpu.VMEM((ENS, 512), BF16),
            pltpu.VMEM((ENS, 256), BF16),
            pltpu.VMEM((ENS, 256), BF16),
            pltpu.VMEM((3, 256, 256), F32),
            pltpu.VMEM((2, 3, 256, 256), F32),
            pltpu.VMEM((2, 3, 256, 256), F32),
            pltpu.VMEM((2, 8, ENS), F32),
            pltpu.VMEM((2, 8, ENS), F32),
            pltpu.VMEM((3, 8, CELLS), F32),
        ]
        + [half] * 12
        + [full] * 2
        + [
            pltpu.VMEM((ENS, 768), BF16),
            pltpu.VMEM((ENS, 768), BF16),
            pltpu.VMEM((3, ENS, CELLS), F32),
            pltpu.VMEM((8, 768), F32),
            dma((11,)),
            dma((2, 8)),
            dma((2, 8)),
            dma((9, 8)),
            dma((9, 8)),
            dma((8,)),
            dma((8,)),
            dma((2, 6)),
            dma((2, 6)),
            dma((2, 8)),
            dma((2, 8)),
        ],
        compiler_params=pltpu.CompilerParams(
            collective_id=0, has_side_effects=True, vmem_limit_bytes=40 << 20
        ),
        name="letkf_cycle",
    )(*(pltpu.with_memory_space_constraint(a, pltpu.HBM) for a in (ensemble_state, obs_cell, obs_value, obs_prec)))
    return pl.pallas_call(
        unpack,
        out_shape=jax.ShapeDtypeStruct((3, LOC, ROWS, LON), F32),
        in_specs=[vmem, vmem],
        out_specs=pl.BlockSpec(memory_space=pl.ANY),
        scratch_shapes=[pltpu.VMEM((3, LOC, ROWS, LON), F32), dma((8,))],
        compiler_params=pltpu.CompilerParams(vmem_limit_bytes=16 << 20),
        name="unpack",
    )(received, biases)


def solution(mesh):
    in_specs = (P(None, "member", "lat", None), P(), P(), P())
    out_specs = P(None, "member", "lat", None)
    return jax.shard_map(body, mesh=mesh, in_specs=in_specs, out_specs=out_specs, check_vma=False)
```

```python
import math

import jax
import jax.numpy as jnp
from jax import lax
from jax.experimental import pallas as pl
from jax.experimental.pallas import tpu as pltpu
from jax.sharding import PartitionSpec as P

MESH = pl.DeviceIdType.MESH
F32 = jnp.float32
BF16 = jnp.bfloat16
NM = 8
NL = 16
ENS = 512
LOC = 64
ROWS = 8
LON = 256
CELLS = 256
DT = 0.3
NN = (((1,), (0,)), ((), ()))
NT = (((1,), (1,)), ((), ()))
BLOCKS = ((0, 0), (0, 1), (1, 1))


def dot(a, b, dims=NN):
    return lax.dot_general(a, b, dims, preferred_element_type=F32)


def split(v):
    high = v.astype(BF16)
    low = (v - high.astype(F32)).astype(BF16)
    return high, low


def iota(shape, dim):
    return lax.broadcasted_iota(jnp.int32, shape, dim)


def exchange_lanes(v, halves, evens):
    a0 = jnp.where(halves, v[0], pltpu.roll(v[2], 64, 1))
    a2 = jnp.where(halves, pltpu.roll(v[0], 64, 1), v[2])
    a1 = jnp.where(halves, v[1], pltpu.roll(v[3], 64, 1))
    a3 = jnp.where(halves, pltpu.roll(v[1], 64, 1), v[3])
    o0 = jnp.where(evens, a0, pltpu.roll(a1, 32, 1))
    o1 = jnp.where(evens, pltpu.roll(a0, 96, 1), a1)
    o2 = jnp.where(evens, a2, pltpu.roll(a3, 32, 1))
    o3 = jnp.where(evens, pltpu.roll(a2, 96, 1), a3)
    return [o0, o1, o2, o3]


def row_times(row, mat_h, mat_l, dims=NN):
    high = row.astype(BF16).astype(F32)
    lhs = jnp.concatenate([high, row - high, jnp.zeros((6, row.shape[1]), F32)], axis=0)
    lhs = lhs.astype(BF16)
    first = dot(lhs, mat_h, dims)
    second = dot(lhs, mat_l, dims)
    return first[0:1] + first[1:2] + second[0:1]


def kernel(
    x_in, cell_in, val_in, prec_in, ro, bo,
    xn, cell, val, prec, xs, ht, hb, rl, pk, rh, xf, sh, sl, s2h, s2l, g0, gs, gr, ds_, dr, co,
    yh, yl, zh, zl, mh, ml, bh, bl, qh, ql, gh, gl, mf, rf, xh, xl, ao, bs,
    in_sem, h_send, h_recv, d_send, d_recv, r_send, o_send, o_recv, f_send, f_recv, g_send, g_recv, a_send, a_recv,
):
    me = lax.axis_index("member")
    lat = lax.axis_index("lat")
    south = lax.rem(lat + 1, NL)
    north = lax.rem(lat + NL - 1, NL)

    def peer(k):
        return lax.rem(me + k, NM)

    def source(k):
        return lax.rem(me + NM - k, NM)

    def state_in(g):
        rows = pl.ds(pl.multiple_of(g * 8, 8), 8)
        return pltpu.make_async_copy(x_in.at[:, rows], xn.at[:, rows], in_sem.at[g])

    obs_in = [
        pltpu.make_async_copy(a.at[lat], b, in_sem.at[8 + i])
        for i, (a, b) in enumerate(((cell_in, cell), (val_in, val), (prec_in, prec)))
    ]
    for g in range(8):
        state_in(g).start()
    for c in obs_in:
        c.start()
    barrier = pltpu.get_barrier_semaphore()
    for k in range(1, NM):
        pl.semaphore_signal(barrier, inc=1, device_id={"member": peer(k)}, device_id_type=MESH)
    for there in (north, south):
        pl.semaphore_signal(barrier, inc=1, device_id={"lat": there}, device_id_type=MESH)
    across = lax.rem(lat + NL // 2, NL)
    mirrored = jnp.where(lat < NL // 2, NL // 2 - 1 - lat, 3 * NL // 2 - 1 - lat)
    at_edge = (lat == 0) | (lat == NL - 1)
    at_middle = (lat == NL // 2 - 1) | (lat == NL // 2)
    at_corner = at_edge | at_middle

    @pl.when(at_corner)
    def _():
        for there in (across, mirrored):
            pl.semaphore_signal(barrier, inc=1, device_id={"lat": there}, device_id_type=MESH)


    def halo(side, g):
        rows = pl.ds(pl.multiple_of(g * 8, 8), 8)
        src = xs.at[:, 0:4, rows, :] if side == 0 else xs.at[:, 4:8, rows, :]
        dst = (hb if side == 0 else ht).at[:, :, rows, :]
        return pltpu.make_async_remote_copy(
            src_ref=src, dst_ref=dst, send_sem=h_send.at[side, g], recv_sem=h_recv.at[side, g],
            device_id={"lat": north if side == 0 else south}, device_id_type=MESH,
        )

    has_north, has_south = lat > 0, lat < NL - 1

    def detour(side, g):
        rows = pl.ds(pl.multiple_of(g * 8, 8), 8)
        src = xs.at[:, 0:4, rows, :] if side == 0 else xs.at[:, 4:8, rows, :]
        return pltpu.make_async_remote_copy(
            src_ref=src, dst_ref=rl.at[:, :, rows, :], send_sem=d_send.at[g], recv_sem=d_recv.at[g],
            device_id={"lat": across}, device_id_type=MESH,
        )

    def relay(side, g):
        rows = pl.ds(pl.multiple_of(g * 8, 8), 8)
        dst = (hb if side == 0 else ht).at[:, :, rows, :]
        return pltpu.make_async_remote_copy(
            src_ref=rl.at[:, :, rows, :], dst_ref=dst, send_sem=r_send.at[g], recv_sem=h_recv.at[side, g],
            device_id={"lat": mirrored}, device_id_type=MESH,
        )


    with jax.named_scope("barrier"):

        @pl.when(at_corner)
        def _():
            pl.semaphore_wait(barrier, NM + 3)

        @pl.when(jnp.logical_not(at_corner))
        def _():
            pl.semaphore_wait(barrier, NM + 1)

    with jax.named_scope("load"):

        @pl.loop(0, 8)
        def _(g):
            state_in(g).wait()
            rows = pl.ds(pl.multiple_of(g * 8, 8), 8)
            for f in range(3):
                for r in range(ROWS):
                    xs[f, r, rows, :] = xn[f, rows, r, :]

            by_relay = lax.rem(g, 2) == 1

            @pl.when(has_north & jnp.logical_not((lat == NL // 2) & by_relay))
            def _():
                halo(0, g).start()

            @pl.when(has_south & jnp.logical_not((lat == NL // 2 - 1) & by_relay))
            def _():
                halo(1, g).start()

            @pl.when((lat == NL // 2) & by_relay)
            def _():
                detour(0, g).start()

            @pl.when((lat == NL // 2 - 1) & by_relay)
            def _():
                detour(1, g).start()

    @pl.when(lat == 0)
    def _():
        ht[...] = jnp.zeros((3, 4, LOC, LON), F32)

    @pl.when(lat == NL - 1)
    def _():
        hb[...] = jnp.zeros((3, 4, LOC, LON), F32)

    for c in obs_in:
        c.wait()
    cells_at = iota((CELLS, CELLS), 0)
    for b in range(3):
        q = me + (b - 1)
        q_in = jnp.clip(q, 0, NM - 1)
        there = ((q >= 0) & (q < NM)).astype(jnp.int32).astype(F32)
        c_row = cell[pl.ds(q_in, 1), :]
        p_row = prec[pl.ds(q_in, 1), :] * there
        v_row = val[pl.ds(q_in, 1), :] * p_row
        parts = []
        for r in (p_row, v_row):
            one = r.astype(BF16).astype(F32)
            two = (r - one).astype(BF16).astype(F32)
            parts += [one, two, r - one - two]
        lhs = jnp.concatenate(parts + [jnp.zeros((2, CELLS), F32)], axis=0).astype(BF16)
        hot = jnp.where(cells_at == c_row, 1.0, 0.0).astype(BF16)
        sums = dot(lhs, hot, NT)
        p_sum = sums[0:1] + sums[1:2] + sums[2:3]
        v_sum = sums[3:4] + sums[4:5] + sums[5:6]
        root = jnp.sqrt(p_sum)
        co[b, 0:1, :] = root
        co[b, 1:2, :] = jnp.where(p_sum > 0.0, v_sum / jnp.where(p_sum > 0.0, root, 1.0), 0.0)

    lane = iota((8, LON), 1)
    west_edge = lane == 0
    east_edge = lane == LON - 1
    lane1 = iota((8, 128), 1)
    halves = lane1 < 64
    evens = (lane1 & 32) == 0
    in_north = jnp.minimum(lat, 1).astype(F32)
    in_south = jnp.minimum(NL - 1 - lat, 1).astype(F32)

    def mask_row(r, state):
        if r < 0:
            return [s * in_north for s in state]
        if r >= ROWS:
            return [s * in_south for s in state]
        return state

    def slope(q):
        east = jnp.where(east_edge, 0.0, pltpu.roll(q, LON - 1, 1))
        west = jnp.where(west_edge, 0.0, pltpu.roll(q, 1, 1))
        return east - west

    half = 0.5 * DT

    def euler(states, r):
        h, u, v = states[r]
        above, below = states[r - 1], states[r + 1]
        spin = DT * (0.5 + ((lat * ROWS + r).astype(F32) * (1.0 / (NL * ROWS)) - 0.5))
        nh = h - half * (slope(u) + (below[2] - above[2]))
        nu = u - half * slope(h) + spin * v
        nv = v - half * (below[0] - above[0]) - spin * u
        return mask_row(r, [nh, nu, nv])

    pk[0, 0, :, :] = jnp.zeros((LOC, CELLS), F32)

    @pl.when(me == NM - 1)
    def _():
        rh[2] = jnp.zeros((ENS, CELLS), F32)

    def obs_copy(g, k, mine):
        d = peer(k)
        src = pk.at[0, pl.ds(d, 2), pl.ds(pl.multiple_of(g * 8, 8), 8), :]
        owner = me if mine else source(k)
        dst = rh.at[0:2, pl.ds(pl.multiple_of(owner * LOC + g * 8, 8), 8), :]
        return pltpu.make_async_remote_copy(
            src_ref=src, dst_ref=dst, send_sem=o_send.at[g, k], recv_sem=o_recv.at[g, k],
            device_id={"member": d}, device_id_type=MESH,
        )

    def east_copy(k, mine):
        d = peer(k)
        owner = me if mine else source(k)
        return pltpu.make_async_remote_copy(
            src_ref=pk.at[0, d + 2, :, :],
            dst_ref=rh.at[2, pl.ds(pl.multiple_of(owner * LOC, LOC), LOC), :],
            send_sem=o_send.at[8, k], recv_sem=o_recv.at[8, k],
            device_id={"member": d}, device_id_type=MESH,
        )

    far_first = (4, 2, 6, 3, 5, 1, 7)

    @pl.loop(0, 8)
    def _(g):

        @pl.when(at_edge & (lax.rem(g, 2) == 1))
        def _():
            detour(0, g).wait_recv()

            @pl.when(lat == 0)
            def _():
                relay(0, g).start()

            @pl.when(lat > 0)
            def _():
                relay(1, g).start()

        @pl.when(has_south)
        def _():
            halo(0, g).wait_recv()

        @pl.when(has_north)
        def _():
            halo(1, g).wait_recv()

        rows = pl.ds(pl.multiple_of(g * 8, 8), 8)

        def start_row(r):
            if r < 0:
                vals = [ht[f, r + 4, rows, :] for f in range(3)]
            elif r >= ROWS:
                vals = [hb[f, r - ROWS, rows, :] for f in range(3)]
            else:
                vals = [xs[f, r, rows, :] for f in range(3)]
            return vals

        s0, m1, s1, m2, s2 = {}, {}, {}, {}, {}
        for r in range(-4, 12):
            s0[r] = start_row(r)
            if r - 1 >= -3:
                m1[r - 1] = euler(s0, r - 1)
            if r - 2 >= -2:
                nxt = euler(m1, r - 2)
                s1[r - 2] = [0.5 * (a + b) for a, b in zip(s0[r - 2], nxt)]
            if r - 3 >= -1:
                m2[r - 3] = euler(s1, r - 3)
            if r - 4 >= 0:
                nxt = euler(m2, r - 4)
                s2[r - 4] = [0.5 * (a + b) for a, b in zip(s1[r - 4], nxt)]
        for f in range(3):
            for t in range(2):
                for rg in range(2):
                    v = [s2[rg * 4 + j][f][:, t * 128 : (t + 1) * 128] for j in range(4)]
                    o = exchange_lanes(v, halves, evens)
                    for b in range(4):
                        pk[f, 1 + 4 * t + b, rows, rg * 128 : (rg + 1) * 128] = o[b]
        mine = pl.ds(pl.multiple_of(me * LOC + g * 8, 8), 8)
        for b in range(2):
            rh[b, mine, :] = pk[0, me + b, rows, :]
        for k in far_first:
            obs_copy(g, k, True).start()

    def field_copy(k, mine):
        d = peer(k)
        owner = me if mine else source(k)
        return pltpu.make_async_remote_copy(
            src_ref=pk.at[1:3, 1 + d, :, :],
            dst_ref=xf.at[:, pl.ds(pl.multiple_of(owner * LOC, LOC), LOC), :],
            send_sem=f_send.at[k], recv_sem=f_recv.at[k],
            device_id={"member": d}, device_id_type=MESH,
        )

    for k in far_first:

        @pl.when(peer(k) < NM - 1)
        def _():
            east_copy(k, True).start()

    own = pl.ds(pl.multiple_of(me * LOC, LOC), LOC)
    for f in range(2):
        xf[f, own, :] = pk[1 + f, 1 + me, :, :]

    @pl.when(me < NM - 1)
    def _():
        rh[2, own, :] = pk[0, me + 2, :, :]

    with jax.named_scope("obs01"):

        @pl.loop(0, 8)
        def _(g):
            for k in range(1, NM):
                obs_copy(g, k, False).wait_recv()

    odd = lax.rem(lat, 2)
    first_peer = lax.rem(lat + NL - 1 + 2 * odd, NL)
    second_peer = lax.rem(lat + NL + 1 - 2 * odd, NL)
    odd_f = odd.astype(F32)
    shifts = (2.0 * odd_f - 1.0, 1.0 - 2.0 * odd_f, 0.0)
    insides = (
        in_north * (1.0 - odd_f) + in_south * odd_f,
        in_south * (1.0 - odd_f) + in_north * odd_f,
        1.0,
    )
    c_at = iota((1, CELLS), 1)
    row_of = (c_at >> 5).astype(F32)
    col_of = (c_at & 31).astype(F32)

    def remote_gram(a, src, dst, n):
        return pltpu.make_async_remote_copy(
            src_ref=src, dst_ref=dst, send_sem=g_send.at[a, n], recv_sem=g_recv.at[a, n],
            device_id={"lat": first_peer if a == 0 else second_peer}, device_id_type=MESH,
        )

    low, top = slice(128, 256), slice(0, 128)
    has_far = has_north & has_south

    def towards(a, act):
        if a == 0:
            pl.when(has_far)(act)
        else:
            act()

    @pl.when((lat == 0) | (lat == NL - 1))
    def _():
        gr[0] = jnp.zeros((3, 256, 256), F32)
        dr[0] = jnp.zeros((8, ENS), F32)

    def gram_copies(a, n):
        if n == 1:
            return [remote_gram(a, gs.at[a, 1], gr.at[a, 1], 2)]
        at = 0 if n == 0 else 3
        return [
            remote_gram(a, gs.at[a, n, top, :], gr.at[a, n, top, :], at),
            remote_gram(a, gs.at[a, n, low, low], gr.at[a, n, low, low], at + 1),
        ]

    def drive_copy(a):
        return remote_gram(a, ds_.at[a], dr.at[a], 5)

    def member_mean(b):
        co[b, 2:3, :] = jnp.sum(rh[b], axis=0, keepdims=True) * (1.0 / ENS)

    def weigh(a, b, to_h, to_l, at):
        up = ((row_of - shifts[a] * ROWS) - 0.5 * (ROWS - 1)) / ROWS
        east = ((col_of + (b - 1) * 32) - 0.5 * 31) / 32
        t_root = jnp.exp(-0.25 * (up * up + east * east)) * insides[a]
        s_w = t_root * co[b, 0:1, :]
        y_bar = co[b, 2:3, :]

        @pl.loop(0, ENS // 64)
        def _(n):
            r = pl.ds(pl.multiple_of(n * 64, 64), 64)
            s_h, s_l = split((rh[b, r, :] - y_bar) * s_w)
            to_h[r, at : at + CELLS] = s_h
            to_l[r, at : at + CELLS] = s_l

        return t_root * (co[b, 1:2, :] - y_bar * co[b, 0:1, :])

    def products(h, l):
        left, right = slice(0, 256), slice(256, 512)
        first = dot(h[left, :], h[left, :], NT) + dot(h[left, :], l[left, :], NT)
        first = first + dot(l[left, :], h[left, :], NT)
        both = dot(h[...], h[right, :], NT) + dot(h[...], l[right, :], NT)
        both = both + dot(l[...], h[right, :], NT)
        return [first, both[left], both[right]]

    for b in range(2):
        member_mean(b)
    drives = []
    def west(a):
        push = [weigh(a, b, sh, sl, b * CELLS) for b in range(2)]
        for n, v in enumerate(products(sh, sl)):
            if a < 2:
                gs[a, n] = v
            else:
                g0[n] = v
        return row_times(jnp.concatenate(push, axis=1), sh[...], sl[...], NT)

    def east(a):
        push = weigh(a, 2, s2h, s2l, 0)
        for n, v in enumerate(products(s2h, s2l)):
            if a < 2:
                gs[a, n] = gs[a, n] + v
            else:
                g0[n] = g0[n] + v

        def send():
            for n in range(3):
                for c in gram_copies(a, n):
                    c.start()

        if a < 2:
            towards(a, send)
        return row_times(push, s2h[...], s2l[...], NT)

    drives = [None] * 3
    with jax.named_scope("gram01"):
        for a in range(2):
            drives[a] = west(a)

    with jax.named_scope("obs2"):

        @pl.when(me < NM - 1)
        def _():
            for k in range(1, NM):
                east_copy(k, False).wait_recv()

    member_mean(2)
    with jax.named_scope("gram2"):
        for a in range(2):
            drives[a] = drives[a] + east(a)
            ds_[a] = jnp.broadcast_to(drives[a], (8, ENS))
            towards(a, lambda a=a: drive_copy(a).start())

    with jax.named_scope("gramown"):
        drives[2] = west(2)
        drives[2] = drives[2] + east(2)

    with jax.named_scope("gwait"):
        for a in range(2):

            def arrive(a=a):
                for n in range(3):
                    for c in gram_copies(a, n):
                        c.wait_recv()
                drive_copy(a).wait_recv()

            towards(a, arrive)
    for k in far_first:
        field_copy(k, True).start()
    drive = drives[2] + dr[0, 0:1, :] + dr[1, 0:1, :]

    squares = jnp.zeros((8, 128), F32)
    for n, (i, j) in enumerate(BLOCKS):
        for part in range(4):
            if i == j and part >= 2:
                lanes = ((part * 64, 128),)
            else:
                lanes = ((0, 0), (0, 128))
            for _unused, c0 in lanes:
                r, c = slice(part * 64, (part + 1) * 64), slice(c0, c0 + 128)
                tot = g0[n, r, c] + gr[0, n, r, c] + gr[1, n, r, c]
                if i == j:
                    on = iota((64, 128), 0) + part * 64 == iota((64, 128), 1) + c0
                    tot = tot + jnp.where(on, ENS - 1.0, 0.0)
                g0[n, r, c] = tot
                sq = jnp.sum((tot * tot).reshape(8, 8, 128), axis=0)
                twice = i != j or (part < 2 and c0 == 128)
                squares = squares + (2.0 * sq if twice else sq)
        if i == j:
            g0[n, low, top] = g0[n, top, low].T
    fro = jnp.sqrt(jnp.sum(squares, axis=(0, 1), keepdims=True))
    inv_fro = 1.0 / fro

    def span(i):
        return slice(i * 256, (i + 1) * 256)

    def put(h, l, i, j, v):
        v_h, v_l = split(v)
        h[span(i), span(j)] = v_h
        l[span(i), span(j)] = v_l
        if i < j:
            h[span(j), span(i)] = v_h.T
            l[span(j), span(i)] = v_l.T

    def mul(a_h, a_l, b_h, b_l, i, j):
        acc = dot(a_h[span(i), :], b_h[:, span(j)]) + dot(a_h[span(i), :], b_l[:, span(j)])
        return acc + dot(a_l[span(i), :], b_h[:, span(j)])

    def eye(i, j, scale):
        if i != j:
            return 0.0
        return jnp.where(iota((256, 256), 0) == iota((256, 256), 1), scale, 0.0)

    def square(a_h, a_l):
        for i, j in BLOCKS:
            m = mf[span(i), span(j)]
            m2 = mul(a_h, a_l, a_h, a_l, i, j)
            put(bh, bl, i, j, m2)
            put(qh, ql, i, j, 0.0625 * m2 - 0.5625 * m)
            rf[span(i), span(j)] = (1.6875 * m2 - 2.4375 * m) + eye(i, j, 2.25)

    def pair_factor(to_h, to_l):
        for i, j in BLOCKS:
            put(to_h, to_l, i, j, rf[span(i), span(j)] + mul(bh, bl, qh, ql, i, j))

    def times(to_h, to_l, a_h, a_l, b_h, b_l):
        new = [mul(a_h, a_l, b_h, b_l, i, j) for i, j in BLOCKS]
        for (i, j), v in zip(BLOCKS, new):
            put(to_h, to_l, i, j, v)

    def take_states(f):
        ref = rh.at[1] if f == 0 else xf.at[f - 1]
        if f == 0:
            bar = co[1, 2:3, :]
        else:
            bar = jnp.sum(ref[...], axis=0, keepdims=True) * (1.0 / ENS)
        bs[0:1, f * CELLS : (f + 1) * CELLS] = bar

        @pl.loop(0, ENS // 64)
        def _(n):
            r = pl.ds(pl.multiple_of(n * 64, 64), 64)
            x_h, x_l = split(ref[r, :] - bar)
            xh[r, f * CELLS : (f + 1) * CELLS] = x_h
            xl[r, f * CELLS : (f + 1) * CELLS] = x_l

    for n, (i, j) in enumerate(BLOCKS):
        scaled = g0[n] * inv_fro
        mf[span(i), span(j)] = scaled
        put(yh, yl, i, j, scaled)
    square(yh, yl)
    pair_factor(zh, zl)
    times(yh, yl, yh, yl, zh, zl)

    def step():
        for i, j in BLOCKS:
            m = mul(zh, zl, yh, yl, i, j)
            mf[span(i), span(j)] = m
            put(mh, ml, i, j, m)
        square(mh, ml)
        pair_factor(gh, gl)

    with jax.named_scope("ns"):

        @pl.loop(0, 4)
        def _(n):
            step()
            times(yh, yl, yh, yl, gh, gl)
            times(zh, zl, gh, gl, zh, zl)

    with jax.named_scope("fields"):
        for k in range(1, NM):
            field_copy(k, False).wait_recv()
    with jax.named_scope("states"):
        for f in range(3):
            take_states(f)

    with jax.named_scope("ns5"):
        step()
        times(zh, zl, gh, gl, zh, zl)
    scale = math.sqrt(ENS - 1.0) / jnp.sqrt(fro)

    def analysis_copy(k, mine):
        d = peer(k)
        owner = me if mine else source(k)
        return pltpu.make_async_remote_copy(
            src_ref=ao.at[:, pl.ds(pl.multiple_of(d * LOC, LOC), LOC), :],
            dst_ref=ro.at[:, owner, :, :],
            send_sem=a_send.at[0, k], recv_sem=a_recv.at[0, k],
            device_id={"member": d}, device_id_type=MESH,
        )

    def analysed(d):
        r = pl.ds(pl.multiple_of(d * LOC, LOC), LOC)
        both = dot(jnp.concatenate([zh[r, :], zl[r, :]], axis=0), xh[...])
        acc = both[0:LOC] + both[LOC : 2 * LOC] + dot(zh[r, :], xl[...])
        return acc * scale

    def bias_copy(k, mine):
        d = peer(k)
        owner = me if mine else source(k)
        return pltpu.make_async_remote_copy(
            src_ref=bs, dst_ref=bo.at[owner],
            send_sem=a_send.at[1, k], recv_sem=a_recv.at[1, k],
            device_id={"member": d}, device_id_type=MESH,
        )


    for k in far_first:
        d = peer(k)
        r = pl.ds(pl.multiple_of(d * LOC, LOC), LOC)
        res = analysed(d)
        for f in range(3):
            ao[f, r, :] = res[:, f * CELLS : (f + 1) * CELLS]
        analysis_copy(k, True).start()
    res = analysed(me)
    for f in range(3):
        ro[f, me, :, :] = res[:, f * CELLS : (f + 1) * CELLS]
    mean_weight = row_times(row_times(drive, zh[...], zl[...]), zh[...], zl[...]) * inv_fro
    bias = bs[0:1, :] + row_times(mean_weight, xh[...], xl[...])
    bs[...] = jnp.broadcast_to(bias, (8, 768))
    bo[me] = jnp.broadcast_to(bias, (8, 768))
    for k in far_first:
        bias_copy(k, True).start()
    with jax.named_scope("out"):
        for k in range(1, NM):
            analysis_copy(k, False).wait_recv()
            bias_copy(k, False).wait_recv()

    @pl.loop(0, 8)
    def _(g):

        by_relay = lax.rem(g, 2) == 1

        @pl.when(has_north & jnp.logical_not((lat == NL // 2) & by_relay))
        def _():
            halo(0, g).wait_send()

        @pl.when(has_south & jnp.logical_not((lat == NL // 2 - 1) & by_relay))
        def _():
            halo(1, g).wait_send()

        @pl.when(at_middle & by_relay)
        def _():
            detour(0, g).wait_send()

        @pl.when(at_edge & by_relay)
        def _():
            relay(0, g).wait_send()

        for k in range(1, NM):
            obs_copy(g, k, True).wait_send()

    for k in range(1, NM):

        @pl.when(peer(k) < NM - 1)
        def _():
            east_copy(k, True).wait_send()

    for k in range(1, NM):
        field_copy(k, True).wait_send()
        analysis_copy(k, True).wait_send()
        bias_copy(k, True).wait_send()
    for a in range(2):

        def left(a=a):
            for n in range(3):
                for c in gram_copies(a, n):
                    c.wait_send()
            drive_copy(a).wait_send()

        towards(a, left)


def unpack(ro, bo, out, held, sem):
    lane1 = iota((8, 128), 1)
    halves = lane1 < 64
    evens = (lane1 & 32) == 0

    def leave(g):
        rows = pl.ds(pl.multiple_of(g * 8, 8), 8)
        return pltpu.make_async_copy(held.at[:, rows], out.at[:, rows], sem.at[g])

    @pl.loop(0, 8)
    def _(g):
        rows = pl.ds(pl.multiple_of(g * 8, 8), 8)
        for f in range(3):
            for t in range(2):
                for rg in range(2):
                    at = f * CELLS + rg * 128
                    v = [
                        ro[f, 4 * t + b, rows, rg * 128 : (rg + 1) * 128]
                        + bo[4 * t + b, :, at : at + 128]
                        for b in range(4)
                    ]
                    o = exchange_lanes(v, halves, evens)
                    for j in range(4):
                        held[f, rows, rg * 4 + j, t * 128 : (t + 1) * 128] = o[j]
        leave(g).start()

    for g in range(8):
        leave(g).wait()


def body(ensemble_state, obs_cell, obs_value, obs_prec):
    vmem = pl.BlockSpec(memory_space=pltpu.VMEM)
    anywhere = pl.BlockSpec(memory_space=pltpu.HBM)
    half = pltpu.VMEM((ENS, ENS), BF16)
    full = pltpu.VMEM((ENS, ENS), F32)
    dma = pltpu.SemaphoreType.DMA
    received, biases = pl.pallas_call(
        kernel,
        out_shape=(
            jax.ShapeDtypeStruct((3, NM, LOC, CELLS), F32),
            jax.ShapeDtypeStruct((NM, 8, 768), F32),
        ),
        in_specs=[anywhere] * 4,
        out_specs=(vmem, vmem),
        scratch_shapes=[
            pltpu.VMEM((3, LOC, ROWS, LON), F32),
            pltpu.VMEM((8, 256), jnp.int32),
            pltpu.VMEM((8, 256), F32),
            pltpu.VMEM((8, 256), F32),
            pltpu.VMEM((3, ROWS, LOC, LON), F32),
            pltpu.VMEM((3, 4, LOC, LON), F32),
            pltpu.VMEM((3, 4, LOC, LON), F32),
            pltpu.VMEM((3, 4, LOC, LON), F32),
            pltpu.VMEM((3, 10, LOC, CELLS), F32),
            pltpu.VMEM((3, ENS, CELLS), F32),
            pltpu.VMEM((2, ENS, CELLS), F32),
            pltpu.VMEM((ENS, 512), BF16),
            pltpu.VMEM((ENS, 512), BF16),
            pltpu.VMEM((ENS, 256), BF16),
            pltpu.VMEM((ENS, 256), BF16),
            pltpu.VMEM((3, 256, 256), F32),
            pltpu.VMEM((2, 3, 256, 256), F32),
            pltpu.VMEM((2, 3, 256, 256), F32),
            pltpu.VMEM((2, 8, ENS), F32),
            pltpu.VMEM((2, 8, ENS), F32),
            pltpu.VMEM((3, 8, CELLS), F32),
        ]
        + [half] * 12
        + [full] * 2
        + [
            pltpu.VMEM((ENS, 768), BF16),
            pltpu.VMEM((ENS, 768), BF16),
            pltpu.VMEM((3, ENS, CELLS), F32),
            pltpu.VMEM((8, 768), F32),
            dma((11,)),
            dma((2, 8)),
            dma((2, 8)),
            dma((8,)),
            dma((8,)),
            dma((8,)),
            dma((9, 8)),
            dma((9, 8)),
            dma((8,)),
            dma((8,)),
            dma((2, 6)),
            dma((2, 6)),
            dma((2, 8)),
            dma((2, 8)),
        ],
        compiler_params=pltpu.CompilerParams(
            collective_id=0, has_side_effects=True, vmem_limit_bytes=40 << 20
        ),
        name="letkf_cycle",
    )(*(pltpu.with_memory_space_constraint(a, pltpu.HBM) for a in (ensemble_state, obs_cell, obs_value, obs_prec)))
    return pl.pallas_call(
        unpack,
        out_shape=jax.ShapeDtypeStruct((3, LOC, ROWS, LON), F32),
        in_specs=[vmem, vmem],
        out_specs=pl.BlockSpec(memory_space=pl.ANY),
        scratch_shapes=[pltpu.VMEM((3, LOC, ROWS, LON), F32), dma((8,))],
        compiler_params=pltpu.CompilerParams(vmem_limit_bytes=16 << 20),
        name="unpack",
    )(received, biases)


def solution(mesh):
    in_specs = (P(None, "member", "lat", None), P(), P(), P())
    out_specs = P(None, "member", "lat", None)
    return jax.shard_map(body, mesh=mesh, in_specs=in_specs, out_specs=out_specs, check_vma=False)
```

```python
import math

import jax
import jax.numpy as jnp
from jax import lax
from jax.experimental import pallas as pl
from jax.experimental.pallas import tpu as pltpu
from jax.sharding import PartitionSpec as P

MESH = pl.DeviceIdType.MESH
F32 = jnp.float32
BF16 = jnp.bfloat16
NM = 8
NL = 16
ENS = 512
LOC = 64
ROWS = 8
LON = 256
CELLS = 256
DT = 0.3
NN = (((1,), (0,)), ((), ()))
NT = (((1,), (1,)), ((), ()))
BLOCKS = ((0, 0), (0, 1), (1, 1))


def dot(a, b, dims=NN):
    return lax.dot_general(a, b, dims, preferred_element_type=F32)


def split(v):
    high = v.astype(BF16)
    low = (v - high.astype(F32)).astype(BF16)
    return high, low


def iota(shape, dim):
    return lax.broadcasted_iota(jnp.int32, shape, dim)


def exchange_lanes(v, halves, evens):
    a0 = jnp.where(halves, v[0], pltpu.roll(v[2], 64, 1))
    a2 = jnp.where(halves, pltpu.roll(v[0], 64, 1), v[2])
    a1 = jnp.where(halves, v[1], pltpu.roll(v[3], 64, 1))
    a3 = jnp.where(halves, pltpu.roll(v[1], 64, 1), v[3])
    o0 = jnp.where(evens, a0, pltpu.roll(a1, 32, 1))
    o1 = jnp.where(evens, pltpu.roll(a0, 96, 1), a1)
    o2 = jnp.where(evens, a2, pltpu.roll(a3, 32, 1))
    o3 = jnp.where(evens, pltpu.roll(a2, 96, 1), a3)
    return [o0, o1, o2, o3]


def row_times(row, mat_h, mat_l, dims=NN):
    high = row.astype(BF16).astype(F32)
    lhs = jnp.concatenate([high, row - high, jnp.zeros((6, row.shape[1]), F32)], axis=0)
    lhs = lhs.astype(BF16)
    first = dot(lhs, mat_h, dims)
    second = dot(lhs, mat_l, dims)
    return first[0:1] + first[1:2] + second[0:1]


def kernel(
    x_in, cell_in, val_in, prec_in, ro, bo,
    xn, cell, val, prec, xs, ht, hb, rl, pk, rh, xf, sh, sl, s2h, s2l, g0, gs, gr, ds_, dr, co,
    yh, yl, zh, zl, mh, ml, bh, bl, qh, ql, gh, gl, mf, rf, xh, xl, ao, bs,
    in_sem, h_send, h_recv, d_send, d_recv, r_send, o_send, o_recv, f_send, f_recv, g_send, g_recv, a_send, a_recv,
):
    me = lax.axis_index("member")
    lat = lax.axis_index("lat")
    south = lax.rem(lat + 1, NL)
    north = lax.rem(lat + NL - 1, NL)

    def peer(k):
        return lax.rem(me + k, NM)

    def source(k):
        return lax.rem(me + NM - k, NM)

    def state_in(g):
        rows = pl.ds(pl.multiple_of(g * 8, 8), 8)
        return pltpu.make_async_copy(x_in.at[:, rows], xn.at[:, rows], in_sem.at[g])

    obs_in = [
        pltpu.make_async_copy(a.at[lat], b, in_sem.at[8 + i])
        for i, (a, b) in enumerate(((cell_in, cell), (val_in, val), (prec_in, prec)))
    ]
    for g in range(8):
        state_in(g).start()
    for c in obs_in:
        c.start()
    barrier = pltpu.get_barrier_semaphore()
    for k in range(1, NM):
        pl.semaphore_signal(barrier, inc=1, device_id={"member": peer(k)}, device_id_type=MESH)
    for there in (north, south):
        pl.semaphore_signal(barrier, inc=1, device_id={"lat": there}, device_id_type=MESH)
    across = lax.rem(lat + NL // 2, NL)
    mirrored = jnp.where(lat < NL // 2, NL // 2 - 1 - lat, 3 * NL // 2 - 1 - lat)
    at_edge = (lat == 0) | (lat == NL - 1)
    at_middle = (lat == NL // 2 - 1) | (lat == NL // 2)
    at_corner = at_edge | at_middle

    @pl.when(at_corner)
    def _():
        for there in (across, mirrored):
            pl.semaphore_signal(barrier, inc=1, device_id={"lat": there}, device_id_type=MESH)


    def halo(side, g):
        rows = pl.ds(pl.multiple_of(g * 8, 8), 8)
        src = xs.at[:, 0:4, rows, :] if side == 0 else xs.at[:, 4:8, rows, :]
        dst = (hb if side == 0 else ht).at[:, :, rows, :]
        return pltpu.make_async_remote_copy(
            src_ref=src, dst_ref=dst, send_sem=h_send.at[side, g], recv_sem=h_recv.at[side, g],
            device_id={"lat": north if side == 0 else south}, device_id_type=MESH,
        )

    has_north, has_south = lat > 0, lat < NL - 1

    def detour(side, g):
        rows = pl.ds(pl.multiple_of(g * 8, 8), 8)
        src = xs.at[:, 0:4, rows, :] if side == 0 else xs.at[:, 4:8, rows, :]
        return pltpu.make_async_remote_copy(
            src_ref=src, dst_ref=rl.at[:, :, rows, :], send_sem=d_send.at[g], recv_sem=d_recv.at[g],
            device_id={"lat": across}, device_id_type=MESH,
        )

    def relay(side, g):
        rows = pl.ds(pl.multiple_of(g * 8, 8), 8)
        dst = (hb if side == 0 else ht).at[:, :, rows, :]
        return pltpu.make_async_remote_copy(
            src_ref=rl.at[:, :, rows, :], dst_ref=dst, send_sem=r_send.at[g], recv_sem=h_recv.at[side, g],
            device_id={"lat": mirrored}, device_id_type=MESH,
        )


    with jax.named_scope("barrier"):

        @pl.when(at_corner)
        def _():
            pl.semaphore_wait(barrier, NM + 3)

        @pl.when(jnp.logical_not(at_corner))
        def _():
            pl.semaphore_wait(barrier, NM + 1)

    with jax.named_scope("load"):

        @pl.loop(0, 8)
        def _(g):
            state_in(g).wait()
            rows = pl.ds(pl.multiple_of(g * 8, 8), 8)
            for f in range(3):
                for r in range(ROWS):
                    xs[f, r, rows, :] = xn[f, rows, r, :]

            by_relay = lax.rem(g, 2) == 1

            @pl.when(has_north & jnp.logical_not((lat == NL // 2) & by_relay))
            def _():
                halo(0, g).start()

            @pl.when(has_south & jnp.logical_not((lat == NL // 2 - 1) & by_relay))
            def _():
                halo(1, g).start()

            @pl.when((lat == NL // 2) & by_relay)
            def _():
                detour(0, g).start()

            @pl.when((lat == NL // 2 - 1) & by_relay)
            def _():
                detour(1, g).start()

    @pl.when(lat == 0)
    def _():
        ht[...] = jnp.zeros((3, 4, LOC, LON), F32)

    @pl.when(lat == NL - 1)
    def _():
        hb[...] = jnp.zeros((3, 4, LOC, LON), F32)

    for c in obs_in:
        c.wait()
    cells_at = iota((CELLS, CELLS), 0)
    for b in range(3):
        q = me + (b - 1)
        q_in = jnp.clip(q, 0, NM - 1)
        there = ((q >= 0) & (q < NM)).astype(jnp.int32).astype(F32)
        c_row = cell[pl.ds(q_in, 1), :]
        p_row = prec[pl.ds(q_in, 1), :] * there
        v_row = val[pl.ds(q_in, 1), :] * p_row
        parts = []
        for r in (p_row, v_row):
            one = r.astype(BF16).astype(F32)
            two = (r - one).astype(BF16).astype(F32)
            parts += [one, two, r - one - two]
        lhs = jnp.concatenate(parts + [jnp.zeros((2, CELLS), F32)], axis=0).astype(BF16)
        hot = jnp.where(cells_at == c_row, 1.0, 0.0).astype(BF16)
        sums = dot(lhs, hot, NT)
        p_sum = sums[0:1] + sums[1:2] + sums[2:3]
        v_sum = sums[3:4] + sums[4:5] + sums[5:6]
        root = jnp.sqrt(p_sum)
        co[b, 0:1, :] = root
        co[b, 1:2, :] = jnp.where(p_sum > 0.0, v_sum / jnp.where(p_sum > 0.0, root, 1.0), 0.0)

    lane = iota((8, LON), 1)
    west_edge = lane == 0
    east_edge = lane == LON - 1
    lane1 = iota((8, 128), 1)
    halves = lane1 < 64
    evens = (lane1 & 32) == 0
    in_north = jnp.minimum(lat, 1).astype(F32)
    in_south = jnp.minimum(NL - 1 - lat, 1).astype(F32)

    def mask_row(r, state):
        if r < 0:
            return [s * in_north for s in state]
        if r >= ROWS:
            return [s * in_south for s in state]
        return state

    def slope(q):
        east = jnp.where(east_edge, 0.0, pltpu.roll(q, LON - 1, 1))
        west = jnp.where(west_edge, 0.0, pltpu.roll(q, 1, 1))
        return east - west

    half = 0.5 * DT

    def euler(states, r):
        h, u, v = states[r]
        above, below = states[r - 1], states[r + 1]
        spin = DT * (0.5 + ((lat * ROWS + r).astype(F32) * (1.0 / (NL * ROWS)) - 0.5))
        nh = h - half * (slope(u) + (below[2] - above[2]))
        nu = u - half * slope(h) + spin * v
        nv = v - half * (below[0] - above[0]) - spin * u
        return mask_row(r, [nh, nu, nv])

    pk[0, 0, :, :] = jnp.zeros((LOC, CELLS), F32)

    @pl.when(me == NM - 1)
    def _():
        rh[2] = jnp.zeros((ENS, CELLS), F32)

    def obs_copy(g, k, mine):
        d = peer(k)
        src = pk.at[0, pl.ds(d, 2), pl.ds(pl.multiple_of(g * 8, 8), 8), :]
        owner = me if mine else source(k)
        dst = rh.at[0:2, pl.ds(pl.multiple_of(owner * LOC + g * 8, 8), 8), :]
        return pltpu.make_async_remote_copy(
            src_ref=src, dst_ref=dst, send_sem=o_send.at[g, k], recv_sem=o_recv.at[g, k],
            device_id={"member": d}, device_id_type=MESH,
        )

    def east_copy(k, mine):
        d = peer(k)
        owner = me if mine else source(k)
        return pltpu.make_async_remote_copy(
            src_ref=pk.at[0, d + 2, :, :],
            dst_ref=rh.at[2, pl.ds(pl.multiple_of(owner * LOC, LOC), LOC), :],
            send_sem=o_send.at[8, k], recv_sem=o_recv.at[8, k],
            device_id={"member": d}, device_id_type=MESH,
        )

    far_first = (4, 2, 6, 3, 5, 1, 7)

    @pl.loop(0, 8)
    def _(g):

        @pl.when(at_edge & (lax.rem(g, 2) == 1))
        def _():
            detour(0, g).wait_recv()

            @pl.when(lat == 0)
            def _():
                relay(0, g).start()

            @pl.when(lat > 0)
            def _():
                relay(1, g).start()

        @pl.when(has_south)
        def _():
            halo(0, g).wait_recv()

        @pl.when(has_north)
        def _():
            halo(1, g).wait_recv()

        rows = pl.ds(pl.multiple_of(g * 8, 8), 8)

        def start_row(r):
            if r < 0:
                vals = [ht[f, r + 4, rows, :] for f in range(3)]
            elif r >= ROWS:
                vals = [hb[f, r - ROWS, rows, :] for f in range(3)]
            else:
                vals = [xs[f, r, rows, :] for f in range(3)]
            return vals

        s0, m1, s1, m2, s2 = {}, {}, {}, {}, {}
        for r in range(-4, 12):
            s0[r] = start_row(r)
            if r - 1 >= -3:
                m1[r - 1] = euler(s0, r - 1)
            if r - 2 >= -2:
                nxt = euler(m1, r - 2)
                s1[r - 2] = [0.5 * (a + b) for a, b in zip(s0[r - 2], nxt)]
            if r - 3 >= -1:
                m2[r - 3] = euler(s1, r - 3)
            if r - 4 >= 0:
                nxt = euler(m2, r - 4)
                s2[r - 4] = [0.5 * (a + b) for a, b in zip(s1[r - 4], nxt)]
        for f in range(3):
            for t in range(2):
                for rg in range(2):
                    v = [s2[rg * 4 + j][f][:, t * 128 : (t + 1) * 128] for j in range(4)]
                    o = exchange_lanes(v, halves, evens)
                    for b in range(4):
                        pk[f, 1 + 4 * t + b, rows, rg * 128 : (rg + 1) * 128] = o[b]
        mine = pl.ds(pl.multiple_of(me * LOC + g * 8, 8), 8)
        for b in range(2):
            rh[b, mine, :] = pk[0, me + b, rows, :]
        for k in far_first:
            obs_copy(g, k, True).start()

    def field_copy(k, mine):
        d = peer(k)
        owner = me if mine else source(k)
        return pltpu.make_async_remote_copy(
            src_ref=pk.at[1:3, 1 + d, :, :],
            dst_ref=xf.at[:, pl.ds(pl.multiple_of(owner * LOC, LOC), LOC), :],
            send_sem=f_send.at[k], recv_sem=f_recv.at[k],
            device_id={"member": d}, device_id_type=MESH,
        )

    for k in far_first:

        @pl.when(peer(k) < NM - 1)
        def _():
            east_copy(k, True).start()

    own = pl.ds(pl.multiple_of(me * LOC, LOC), LOC)
    for f in range(2):
        xf[f, own, :] = pk[1 + f, 1 + me, :, :]

    @pl.when(me < NM - 1)
    def _():
        rh[2, own, :] = pk[0, me + 2, :, :]

    with jax.named_scope("obs01"):

        @pl.loop(0, 8)
        def _(g):
            for k in range(1, NM):
                obs_copy(g, k, False).wait_recv()

    odd = lax.rem(lat, 2)
    first_peer = lax.rem(lat + NL - 1 + 2 * odd, NL)
    second_peer = lax.rem(lat + NL + 1 - 2 * odd, NL)
    odd_f = odd.astype(F32)
    shifts = (2.0 * odd_f - 1.0, 1.0 - 2.0 * odd_f, 0.0)
    insides = (
        in_north * (1.0 - odd_f) + in_south * odd_f,
        in_south * (1.0 - odd_f) + in_north * odd_f,
        1.0,
    )
    c_at = iota((1, CELLS), 1)
    row_of = (c_at >> 5).astype(F32)
    col_of = (c_at & 31).astype(F32)

    def remote_gram(a, src, dst, n):
        return pltpu.make_async_remote_copy(
            src_ref=src, dst_ref=dst, send_sem=g_send.at[a, n], recv_sem=g_recv.at[a, n],
            device_id={"lat": first_peer if a == 0 else second_peer}, device_id_type=MESH,
        )

    low, top = slice(128, 256), slice(0, 128)
    has_far = has_north & has_south

    def towards(a, act):
        if a == 0:
            pl.when(has_far)(act)
        else:
            act()

    @pl.when((lat == 0) | (lat == NL - 1))
    def _():
        gr[0] = jnp.zeros((3, 256, 256), F32)
        dr[0] = jnp.zeros((8, ENS), F32)

    def gram_copies(a, n):
        if n == 1:
            return [remote_gram(a, gs.at[a, 1], gr.at[a, 1], 2)]
        at = 0 if n == 0 else 3
        return [
            remote_gram(a, gs.at[a, n, top, :], gr.at[a, n, top, :], at),
            remote_gram(a, gs.at[a, n, low, low], gr.at[a, n, low, low], at + 1),
        ]

    def drive_copy(a):
        return remote_gram(a, ds_.at[a], dr.at[a], 5)

    def member_mean(b):
        co[b, 2:3, :] = jnp.sum(rh[b], axis=0, keepdims=True) * (1.0 / ENS)

    def weigh(a, b, to_h, to_l, at):
        up = ((row_of - shifts[a] * ROWS) - 0.5 * (ROWS - 1)) / ROWS
        east = ((col_of + (b - 1) * 32) - 0.5 * 31) / 32
        t_root = jnp.exp(-0.25 * (up * up + east * east)) * insides[a]
        s_w = t_root * co[b, 0:1, :]
        y_bar = co[b, 2:3, :]

        @pl.loop(0, ENS // 64)
        def _(n):
            r = pl.ds(pl.multiple_of(n * 64, 64), 64)
            s_h, s_l = split((rh[b, r, :] - y_bar) * s_w)
            to_h[r, at : at + CELLS] = s_h
            to_l[r, at : at + CELLS] = s_l

        return t_root * (co[b, 1:2, :] - y_bar * co[b, 0:1, :])

    def products(h, l):
        left, right = slice(0, 256), slice(256, 512)
        first = dot(h[left, :], h[left, :], NT) + dot(h[left, :], l[left, :], NT)
        first = first + dot(l[left, :], h[left, :], NT)
        both = dot(h[...], h[right, :], NT) + dot(h[...], l[right, :], NT)
        both = both + dot(l[...], h[right, :], NT)
        return [first, both[left], both[right]]

    for b in range(2):
        member_mean(b)
    drives = []
    def west(a):
        push = [weigh(a, b, sh, sl, b * CELLS) for b in range(2)]
        for n, v in enumerate(products(sh, sl)):
            if a < 2:
                gs[a, n] = v
            else:
                g0[n] = v
        return row_times(jnp.concatenate(push, axis=1), sh[...], sl[...], NT)

    def east(a):
        push = weigh(a, 2, s2h, s2l, 0)
        left, right = slice(0, 256), slice(256, 512)

        def keep(n, v):
            if a == 2:
                g0[n] = g0[n] + v
                return
            gs[a, n] = gs[a, n] + v

            def send():
                for c in gram_copies(a, n):
                    c.start()

            towards(a, send)

        first = dot(s2h[left, :], s2h[left, :], NT) + dot(s2h[left, :], s2l[left, :], NT)
        keep(0, first + dot(s2l[left, :], s2h[left, :], NT))
        both = dot(s2h[...], s2h[right, :], NT) + dot(s2h[...], s2l[right, :], NT)
        both = both + dot(s2l[...], s2h[right, :], NT)
        keep(1, both[left])
        keep(2, both[right])
        return row_times(push, s2h[...], s2l[...], NT)

    drives = [None] * 3
    with jax.named_scope("gram01"):
        for a in range(2):
            drives[a] = west(a)

    with jax.named_scope("obs2"):

        @pl.when(me < NM - 1)
        def _():
            for k in range(1, NM):
                east_copy(k, False).wait_recv()

    member_mean(2)
    with jax.named_scope("gram2"):
        for a in range(2):
            drives[a] = drives[a] + east(a)
            ds_[a] = jnp.broadcast_to(drives[a], (8, ENS))
            towards(a, lambda a=a: drive_copy(a).start())

    with jax.named_scope("gramown"):
        drives[2] = west(2)
        drives[2] = drives[2] + east(2)

    def take_states(f):
        ref = rh.at[1] if f == 0 else xf.at[f - 1]
        if f == 0:
            bar = co[1, 2:3, :]
        else:
            bar = jnp.sum(ref[...], axis=0, keepdims=True) * (1.0 / ENS)
        bs[0:1, f * CELLS : (f + 1) * CELLS] = bar

        @pl.loop(0, ENS // 64)
        def _(n):
            r = pl.ds(pl.multiple_of(n * 64, 64), 64)
            x_h, x_l = split(ref[r, :] - bar)
            xh[r, f * CELLS : (f + 1) * CELLS] = x_h
            xl[r, f * CELLS : (f + 1) * CELLS] = x_l

    take_states(0)
    with jax.named_scope("gwait"):
        for a in range(2):

            def arrive(a=a):
                for n in range(3):
                    for c in gram_copies(a, n):
                        c.wait_recv()
                drive_copy(a).wait_recv()

            towards(a, arrive)
    for k in far_first:
        field_copy(k, True).start()
    drive = drives[2] + dr[0, 0:1, :] + dr[1, 0:1, :]

    squares = jnp.zeros((8, 128), F32)
    for n, (i, j) in enumerate(BLOCKS):
        for part in range(4):
            if i == j and part >= 2:
                lanes = ((part * 64, 128),)
            else:
                lanes = ((0, 0), (0, 128))
            for _unused, c0 in lanes:
                r, c = slice(part * 64, (part + 1) * 64), slice(c0, c0 + 128)
                tot = g0[n, r, c] + gr[0, n, r, c] + gr[1, n, r, c]
                if i == j:
                    on = iota((64, 128), 0) + part * 64 == iota((64, 128), 1) + c0
                    tot = tot + jnp.where(on, ENS - 1.0, 0.0)
                g0[n, r, c] = tot
                sq = jnp.sum((tot * tot).reshape(8, 8, 128), axis=0)
                twice = i != j or (part < 2 and c0 == 128)
                squares = squares + (2.0 * sq if twice else sq)
        if i == j:
            g0[n, low, top] = g0[n, top, low].T
    fro = jnp.sqrt(jnp.sum(squares, axis=(0, 1), keepdims=True))
    inv_fro = 1.0 / fro

    def span(i):
        return slice(i * 256, (i + 1) * 256)

    def put(h, l, i, j, v):
        v_h, v_l = split(v)
        h[span(i), span(j)] = v_h
        l[span(i), span(j)] = v_l
        if i < j:
            h[span(j), span(i)] = v_h.T
            l[span(j), span(i)] = v_l.T

    def mul(a_h, a_l, b_h, b_l, i, j):
        acc = dot(a_h[span(i), :], b_h[:, span(j)]) + dot(a_h[span(i), :], b_l[:, span(j)])
        return acc + dot(a_l[span(i), :], b_h[:, span(j)])

    def eye(i, j, scale):
        if i != j:
            return 0.0
        return jnp.where(iota((256, 256), 0) == iota((256, 256), 1), scale, 0.0)

    def square(a_h, a_l):
        for i, j in BLOCKS:
            m = mf[span(i), span(j)]
            m2 = mul(a_h, a_l, a_h, a_l, i, j)
            put(bh, bl, i, j, m2)
            put(qh, ql, i, j, 0.0625 * m2 - 0.5625 * m)
            rf[span(i), span(j)] = (1.6875 * m2 - 2.4375 * m) + eye(i, j, 2.25)

    def pair_factor(to_h, to_l):
        for i, j in BLOCKS:
            put(to_h, to_l, i, j, rf[span(i), span(j)] + mul(bh, bl, qh, ql, i, j))

    def times(to_h, to_l, a_h, a_l, b_h, b_l):
        new = [mul(a_h, a_l, b_h, b_l, i, j) for i, j in BLOCKS]
        for (i, j), v in zip(BLOCKS, new):
            put(to_h, to_l, i, j, v)

    for n, (i, j) in enumerate(BLOCKS):
        scaled = g0[n] * inv_fro
        mf[span(i), span(j)] = scaled
        put(yh, yl, i, j, scaled)
    square(yh, yl)
    pair_factor(zh, zl)
    times(yh, yl, yh, yl, zh, zl)

    def step():
        for i, j in BLOCKS:
            m = mul(zh, zl, yh, yl, i, j)
            mf[span(i), span(j)] = m
            put(mh, ml, i, j, m)
        square(mh, ml)
        pair_factor(gh, gl)

    with jax.named_scope("ns"):

        @pl.loop(0, 4)
        def _(n):
            step()
            times(yh, yl, yh, yl, gh, gl)
            times(zh, zl, gh, gl, zh, zl)

    with jax.named_scope("fields"):
        for k in range(1, NM):
            field_copy(k, False).wait_recv()
    with jax.named_scope("states"):
        for f in range(1, 3):
            take_states(f)

    with jax.named_scope("ns5"):
        step()
        times(zh, zl, gh, gl, zh, zl)
    scale = math.sqrt(ENS - 1.0) / jnp.sqrt(fro)

    def analysis_copy(k, mine):
        d = peer(k)
        owner = me if mine else source(k)
        return pltpu.make_async_remote_copy(
            src_ref=ao.at[:, pl.ds(pl.multiple_of(d * LOC, LOC), LOC), :],
            dst_ref=ro.at[:, owner, :, :],
            send_sem=a_send.at[0, k], recv_sem=a_recv.at[0, k],
            device_id={"member": d}, device_id_type=MESH,
        )

    def analysed(d, e):
        r = [pl.ds(pl.multiple_of(i * LOC, LOC), LOC) for i in (d, e)]
        high = jnp.concatenate([zh[i, :] for i in r], axis=0)
        both = dot(jnp.concatenate([high] + [zl[i, :] for i in r], axis=0), xh[...])
        acc = both[0 : 2 * LOC] + both[2 * LOC : 4 * LOC] + dot(high, xl[...])
        return acc * scale

    def bias_copy(k, mine):
        d = peer(k)
        owner = me if mine else source(k)
        return pltpu.make_async_remote_copy(
            src_ref=bs, dst_ref=bo.at[owner],
            send_sem=a_send.at[1, k], recv_sem=a_recv.at[1, k],
            device_id={"member": d}, device_id_type=MESH,
        )


    for pair in ((4, 2), (6, 3), (5, 1), (7, 0)):
        res = analysed(*(peer(k) for k in pair))
        for n, k in enumerate(pair):
            for f in range(3):
                part = res[n * LOC : (n + 1) * LOC, f * CELLS : (f + 1) * CELLS]
                if k:
                    ao[f, pl.ds(pl.multiple_of(peer(k) * LOC, LOC), LOC), :] = part
                else:
                    ro[f, me, :, :] = part
            if k:
                analysis_copy(k, True).start()
    mean_weight = row_times(row_times(drive, zh[...], zl[...]), zh[...], zl[...]) * inv_fro
    bias = bs[0:1, :] + row_times(mean_weight, xh[...], xl[...])
    bs[...] = jnp.broadcast_to(bias, (8, 768))
    bo[me] = jnp.broadcast_to(bias, (8, 768))
    for k in far_first:
        bias_copy(k, True).start()
    with jax.named_scope("out"):
        for k in range(1, NM):
            analysis_copy(k, False).wait_recv()
            bias_copy(k, False).wait_recv()

    @pl.loop(0, 8)
    def _(g):

        by_relay = lax.rem(g, 2) == 1

        @pl.when(has_north & jnp.logical_not((lat == NL // 2) & by_relay))
        def _():
            halo(0, g).wait_send()

        @pl.when(has_south & jnp.logical_not((lat == NL // 2 - 1) & by_relay))
        def _():
            halo(1, g).wait_send()

        @pl.when(at_middle & by_relay)
        def _():
            detour(0, g).wait_send()

        @pl.when(at_edge & by_relay)
        def _():
            relay(0, g).wait_send()

        for k in range(1, NM):
            obs_copy(g, k, True).wait_send()

    for k in range(1, NM):

        @pl.when(peer(k) < NM - 1)
        def _():
            east_copy(k, True).wait_send()

    for k in range(1, NM):
        field_copy(k, True).wait_send()
        analysis_copy(k, True).wait_send()
        bias_copy(k, True).wait_send()
    for a in range(2):

        def left(a=a):
            for n in range(3):
                for c in gram_copies(a, n):
                    c.wait_send()
            drive_copy(a).wait_send()

        towards(a, left)


def unpack(ro, bo, out, held, sem):
    lane1 = iota((8, 128), 1)
    halves = lane1 < 64
    evens = (lane1 & 32) == 0

    def leave(g):
        rows = pl.ds(pl.multiple_of(g * 8, 8), 8)
        return pltpu.make_async_copy(held.at[:, rows], out.at[:, rows], sem.at[g])

    @pl.loop(0, 8)
    def _(g):
        rows = pl.ds(pl.multiple_of(g * 8, 8), 8)
        for f in range(3):
            for t in range(2):
                for rg in range(2):
                    at = f * CELLS + rg * 128
                    v = [
                        ro[f, 4 * t + b, rows, rg * 128 : (rg + 1) * 128]
                        + bo[4 * t + b, :, at : at + 128]
                        for b in range(4)
                    ]
                    o = exchange_lanes(v, halves, evens)
                    for j in range(4):
                        held[f, rows, rg * 4 + j, t * 128 : (t + 1) * 128] = o[j]
        leave(g).start()

    for g in range(8):
        leave(g).wait()


def body(ensemble_state, obs_cell, obs_value, obs_prec):
    vmem = pl.BlockSpec(memory_space=pltpu.VMEM)
    anywhere = pl.BlockSpec(memory_space=pltpu.HBM)
    half = pltpu.VMEM((ENS, ENS), BF16)
    full = pltpu.VMEM((ENS, ENS), F32)
    dma = pltpu.SemaphoreType.DMA
    received, biases = pl.pallas_call(
        kernel,
        out_shape=(
            jax.ShapeDtypeStruct((3, NM, LOC, CELLS), F32),
            jax.ShapeDtypeStruct((NM, 8, 768), F32),
        ),
        in_specs=[anywhere] * 4,
        out_specs=(vmem, vmem),
        scratch_shapes=[
            pltpu.VMEM((3, LOC, ROWS, LON), F32),
            pltpu.VMEM((8, 256), jnp.int32),
            pltpu.VMEM((8, 256), F32),
            pltpu.VMEM((8, 256), F32),
            pltpu.VMEM((3, ROWS, LOC, LON), F32),
            pltpu.VMEM((3, 4, LOC, LON), F32),
            pltpu.VMEM((3, 4, LOC, LON), F32),
            pltpu.VMEM((3, 4, LOC, LON), F32),
            pltpu.VMEM((3, 10, LOC, CELLS), F32),
            pltpu.VMEM((3, ENS, CELLS), F32),
            pltpu.VMEM((2, ENS, CELLS), F32),
            pltpu.VMEM((ENS, 512), BF16),
            pltpu.VMEM((ENS, 512), BF16),
            pltpu.VMEM((ENS, 256), BF16),
            pltpu.VMEM((ENS, 256), BF16),
            pltpu.VMEM((3, 256, 256), F32),
            pltpu.VMEM((2, 3, 256, 256), F32),
            pltpu.VMEM((2, 3, 256, 256), F32),
            pltpu.VMEM((2, 8, ENS), F32),
            pltpu.VMEM((2, 8, ENS), F32),
            pltpu.VMEM((3, 8, CELLS), F32),
        ]
        + [half] * 12
        + [full] * 2
        + [
            pltpu.VMEM((ENS, 768), BF16),
            pltpu.VMEM((ENS, 768), BF16),
            pltpu.VMEM((3, ENS, CELLS), F32),
            pltpu.VMEM((8, 768), F32),
            dma((11,)),
            dma((2, 8)),
            dma((2, 8)),
            dma((8,)),
            dma((8,)),
            dma((8,)),
            dma((9, 8)),
            dma((9, 8)),
            dma((8,)),
            dma((8,)),
            dma((2, 6)),
            dma((2, 6)),
            dma((2, 8)),
            dma((2, 8)),
        ],
        compiler_params=pltpu.CompilerParams(
            collective_id=0, has_side_effects=True, vmem_limit_bytes=40 << 20
        ),
        name="letkf_cycle",
    )(*(pltpu.with_memory_space_constraint(a, pltpu.HBM) for a in (ensemble_state, obs_cell, obs_value, obs_prec)))
    return pl.pallas_call(
        unpack,
        out_shape=jax.ShapeDtypeStruct((3, LOC, ROWS, LON), F32),
        in_specs=[vmem, vmem],
        out_specs=pl.BlockSpec(memory_space=pl.ANY),
        scratch_shapes=[pltpu.VMEM((3, LOC, ROWS, LON), F32), dma((8,))],
        compiler_params=pltpu.CompilerParams(vmem_limit_bytes=16 << 20),
        name="unpack",
    )(received, biases)


def solution(mesh):
    in_specs = (P(None, "member", "lat", None), P(), P(), P())
    out_specs = P(None, "member", "lat", None)
    return jax.shard_map(body, mesh=mesh, in_specs=in_specs, out_specs=out_specs, check_vma=False)
```

```python
import math

import jax
import jax.numpy as jnp
from jax import lax
from jax.experimental import pallas as pl
from jax.experimental.pallas import tpu as pltpu
from jax.sharding import PartitionSpec as P

MESH = pl.DeviceIdType.MESH
F32 = jnp.float32
BF16 = jnp.bfloat16
NM = 8
NL = 16
ENS = 512
LOC = 64
ROWS = 8
LON = 256
CELLS = 256
DT = 0.3
NN = (((1,), (0,)), ((), ()))
NT = (((1,), (1,)), ((), ()))
BLOCKS = ((0, 0), (0, 1), (1, 1))


def dot(a, b, dims=NN):
    return lax.dot_general(a, b, dims, preferred_element_type=F32)


def split(v):
    high = v.astype(BF16)
    low = (v - high.astype(F32)).astype(BF16)
    return high, low


def iota(shape, dim):
    return lax.broadcasted_iota(jnp.int32, shape, dim)


def exchange_lanes(v, halves, evens):
    a0 = jnp.where(halves, v[0], pltpu.roll(v[2], 64, 1))
    a2 = jnp.where(halves, pltpu.roll(v[0], 64, 1), v[2])
    a1 = jnp.where(halves, v[1], pltpu.roll(v[3], 64, 1))
    a3 = jnp.where(halves, pltpu.roll(v[1], 64, 1), v[3])
    o0 = jnp.where(evens, a0, pltpu.roll(a1, 32, 1))
    o1 = jnp.where(evens, pltpu.roll(a0, 96, 1), a1)
    o2 = jnp.where(evens, a2, pltpu.roll(a3, 32, 1))
    o3 = jnp.where(evens, pltpu.roll(a2, 96, 1), a3)
    return [o0, o1, o2, o3]


def row_times(row, mat_h, mat_l, dims=NN):
    high = row.astype(BF16).astype(F32)
    lhs = jnp.concatenate([high, row - high, jnp.zeros((6, row.shape[1]), F32)], axis=0)
    lhs = lhs.astype(BF16)
    first = dot(lhs, mat_h, dims)
    second = dot(lhs, mat_l, dims)
    return first[0:1] + first[1:2] + second[0:1]


def kernel(
    x_in, cell_in, val_in, prec_in, ro, bo,
    xn, cell, val, prec, xs, ht, hb, rl, pk, rh, xf, sh, sl, s2h, s2l, g0, gs, gr, ds_, dr, co,
    yh, yl, zh, zl, mh, ml, bh, bl, qh, ql, gh, gl, mf, rf, xh, xl, ao, bs, bd,
    in_sem, h_send, h_recv, d_send, d_recv, r_send, o_send, o_recv, f_send, f_recv, g_send, g_recv, a_send, a_recv,
):
    me = lax.axis_index("member")
    lat = lax.axis_index("lat")
    south = lax.rem(lat + 1, NL)
    north = lax.rem(lat + NL - 1, NL)

    def peer(k):
        return lax.rem(me + k, NM)

    def source(k):
        return lax.rem(me + NM - k, NM)

    def state_in(g):
        rows = pl.ds(pl.multiple_of(g * 8, 8), 8)
        return pltpu.make_async_copy(x_in.at[:, rows], xn.at[:, rows], in_sem.at[g])

    obs_in = [
        pltpu.make_async_copy(a.at[lat], b, in_sem.at[8 + i])
        for i, (a, b) in enumerate(((cell_in, cell), (val_in, val), (prec_in, prec)))
    ]
    for g in range(8):
        state_in(g).start()
    for c in obs_in:
        c.start()
    barrier = pltpu.get_barrier_semaphore()
    for k in range(1, NM):
        pl.semaphore_signal(barrier, inc=1, device_id={"member": peer(k)}, device_id_type=MESH)
    for there in (north, south):
        pl.semaphore_signal(barrier, inc=1, device_id={"lat": there}, device_id_type=MESH)
    across = lax.rem(lat + NL // 2, NL)
    mirrored = jnp.where(lat < NL // 2, NL // 2 - 1 - lat, 3 * NL // 2 - 1 - lat)
    at_edge = (lat == 0) | (lat == NL - 1)
    at_middle = (lat == NL // 2 - 1) | (lat == NL // 2)
    at_corner = at_edge | at_middle

    @pl.when(at_corner)
    def _():
        for there in (across, mirrored):
            pl.semaphore_signal(barrier, inc=1, device_id={"lat": there}, device_id_type=MESH)


    def halo(side, g):
        rows = pl.ds(pl.multiple_of(g * 8, 8), 8)
        src = xs.at[:, 0:4, rows, :] if side == 0 else xs.at[:, 4:8, rows, :]
        dst = (hb if side == 0 else ht).at[:, :, rows, :]
        return pltpu.make_async_remote_copy(
            src_ref=src, dst_ref=dst, send_sem=h_send.at[side, g], recv_sem=h_recv.at[side, g],
            device_id={"lat": north if side == 0 else south}, device_id_type=MESH,
        )

    has_north, has_south = lat > 0, lat < NL - 1

    def detour(side, g):
        rows = pl.ds(pl.multiple_of(g * 8, 8), 8)
        src = xs.at[:, 0:4, rows, :] if side == 0 else xs.at[:, 4:8, rows, :]
        return pltpu.make_async_remote_copy(
            src_ref=src, dst_ref=rl.at[:, :, rows, :], send_sem=d_send.at[g], recv_sem=d_recv.at[g],
            device_id={"lat": across}, device_id_type=MESH,
        )

    def relay(side, g):
        rows = pl.ds(pl.multiple_of(g * 8, 8), 8)
        dst = (hb if side == 0 else ht).at[:, :, rows, :]
        return pltpu.make_async_remote_copy(
            src_ref=rl.at[:, :, rows, :], dst_ref=dst, send_sem=r_send.at[g], recv_sem=h_recv.at[side, g],
            device_id={"lat": mirrored}, device_id_type=MESH,
        )


    with jax.named_scope("barrier"):

        @pl.when(at_corner)
        def _():
            pl.semaphore_wait(barrier, NM + 3)

        @pl.when(jnp.logical_not(at_corner))
        def _():
            pl.semaphore_wait(barrier, NM + 1)

    with jax.named_scope("load"):

        @pl.loop(0, 8)
        def _(g):
            state_in(g).wait()
            rows = pl.ds(pl.multiple_of(g * 8, 8), 8)
            for f in range(3):
                for r in range(ROWS):
                    xs[f, r, rows, :] = xn[f, rows, r, :]

            by_relay = lax.rem(g, 2) == 1

            @pl.when(has_north & jnp.logical_not((lat == NL // 2) & by_relay))
            def _():
                halo(0, g).start()

            @pl.when(has_south & jnp.logical_not((lat == NL // 2 - 1) & by_relay))
            def _():
                halo(1, g).start()

            @pl.when((lat == NL // 2) & by_relay)
            def _():
                detour(0, g).start()

            @pl.when((lat == NL // 2 - 1) & by_relay)
            def _():
                detour(1, g).start()

    @pl.when(lat == 0)
    def _():
        ht[...] = jnp.zeros((3, 4, LOC, LON), F32)

    @pl.when(lat == NL - 1)
    def _():
        hb[...] = jnp.zeros((3, 4, LOC, LON), F32)

    for c in obs_in:
        c.wait()
    cells_at = iota((CELLS, CELLS), 0)
    for b in range(3):
        q = me + (b - 1)
        q_in = jnp.clip(q, 0, NM - 1)
        there = ((q >= 0) & (q < NM)).astype(jnp.int32).astype(F32)
        c_row = cell[pl.ds(q_in, 1), :]
        p_row = prec[pl.ds(q_in, 1), :] * there
        v_row = val[pl.ds(q_in, 1), :] * p_row
        parts = []
        for r in (p_row, v_row):
            one = r.astype(BF16).astype(F32)
            two = (r - one).astype(BF16).astype(F32)
            parts += [one, two, r - one - two]
        lhs = jnp.concatenate(parts + [jnp.zeros((2, CELLS), F32)], axis=0).astype(BF16)
        hot = jnp.where(cells_at == c_row, 1.0, 0.0).astype(BF16)
        sums = dot(lhs, hot, NT)
        p_sum = sums[0:1] + sums[1:2] + sums[2:3]
        v_sum = sums[3:4] + sums[4:5] + sums[5:6]
        root = jnp.sqrt(p_sum)
        co[b, 0:1, :] = root
        co[b, 1:2, :] = jnp.where(p_sum > 0.0, v_sum / jnp.where(p_sum > 0.0, root, 1.0), 0.0)

    lane = iota((8, LON), 1)
    west_edge = lane == 0
    east_edge = lane == LON - 1
    lane1 = iota((8, 128), 1)
    halves = lane1 < 64
    evens = (lane1 & 32) == 0
    in_north = jnp.minimum(lat, 1).astype(F32)
    in_south = jnp.minimum(NL - 1 - lat, 1).astype(F32)

    def mask_row(r, state):
        if r < 0:
            return [s * in_north for s in state]
        if r >= ROWS:
            return [s * in_south for s in state]
        return state

    def slope(q):
        east = jnp.where(east_edge, 0.0, pltpu.roll(q, LON - 1, 1))
        west = jnp.where(west_edge, 0.0, pltpu.roll(q, 1, 1))
        return east - west

    half = 0.5 * DT

    def euler(states, r):
        h, u, v = states[r]
        above, below = states[r - 1], states[r + 1]
        spin = DT * (0.5 + ((lat * ROWS + r).astype(F32) * (1.0 / (NL * ROWS)) - 0.5))
        nh = h - half * (slope(u) + (below[2] - above[2]))
        nu = u - half * slope(h) + spin * v
        nv = v - half * (below[0] - above[0]) - spin * u
        return mask_row(r, [nh, nu, nv])

    pk[0, 0, :, :] = jnp.zeros((LOC, CELLS), F32)

    @pl.when(me == NM - 1)
    def _():
        rh[2] = jnp.zeros((ENS, CELLS), F32)

    def obs_copy(g, k, mine):
        d = peer(k)
        src = pk.at[0, pl.ds(d, 2), pl.ds(pl.multiple_of(g * 8, 8), 8), :]
        owner = me if mine else source(k)
        dst = rh.at[0:2, pl.ds(pl.multiple_of(owner * LOC + g * 8, 8), 8), :]
        return pltpu.make_async_remote_copy(
            src_ref=src, dst_ref=dst, send_sem=o_send.at[g, k], recv_sem=o_recv.at[g, k],
            device_id={"member": d}, device_id_type=MESH,
        )

    def east_copy(k, mine):
        d = peer(k)
        owner = me if mine else source(k)
        return pltpu.make_async_remote_copy(
            src_ref=pk.at[0, d + 2, :, :],
            dst_ref=rh.at[2, pl.ds(pl.multiple_of(owner * LOC, LOC), LOC), :],
            send_sem=o_send.at[8, k], recv_sem=o_recv.at[8, k],
            device_id={"member": d}, device_id_type=MESH,
        )

    far_first = (4, 2, 6, 3, 5, 1, 7)

    @pl.loop(0, 8)
    def _(g):

        @pl.when(at_edge & (lax.rem(g, 2) == 1))
        def _():
            detour(0, g).wait_recv()

            @pl.when(lat == 0)
            def _():
                relay(0, g).start()

            @pl.when(lat > 0)
            def _():
                relay(1, g).start()

        @pl.when(has_south)
        def _():
            halo(0, g).wait_recv()

        @pl.when(has_north)
        def _():
            halo(1, g).wait_recv()

        rows = pl.ds(pl.multiple_of(g * 8, 8), 8)

        def start_row(r):
            if r < 0:
                vals = [ht[f, r + 4, rows, :] for f in range(3)]
            elif r >= ROWS:
                vals = [hb[f, r - ROWS, rows, :] for f in range(3)]
            else:
                vals = [xs[f, r, rows, :] for f in range(3)]
            return vals

        s0, m1, s1, m2, s2 = {}, {}, {}, {}, {}
        for r in range(-4, 12):
            s0[r] = start_row(r)
            if r - 1 >= -3:
                m1[r - 1] = euler(s0, r - 1)
            if r - 2 >= -2:
                nxt = euler(m1, r - 2)
                s1[r - 2] = [0.5 * (a + b) for a, b in zip(s0[r - 2], nxt)]
            if r - 3 >= -1:
                m2[r - 3] = euler(s1, r - 3)
            if r - 4 >= 0:
                nxt = euler(m2, r - 4)
                s2[r - 4] = [0.5 * (a + b) for a, b in zip(s1[r - 4], nxt)]
        for f in range(3):
            for t in range(2):
                for rg in range(2):
                    v = [s2[rg * 4 + j][f][:, t * 128 : (t + 1) * 128] for j in range(4)]
                    o = exchange_lanes(v, halves, evens)
                    for b in range(4):
                        pk[f, 1 + 4 * t + b, rows, rg * 128 : (rg + 1) * 128] = o[b]
        mine = pl.ds(pl.multiple_of(me * LOC + g * 8, 8), 8)
        for b in range(2):
            rh[b, mine, :] = pk[0, me + b, rows, :]
        for k in far_first:
            obs_copy(g, k, True).start()

    def field_copy(k, mine):
        d = peer(k)
        owner = me if mine else source(k)
        return pltpu.make_async_remote_copy(
            src_ref=pk.at[1:3, 1 + d, :, :],
            dst_ref=xf.at[:, pl.ds(pl.multiple_of(owner * LOC, LOC), LOC), :],
            send_sem=f_send.at[k], recv_sem=f_recv.at[k],
            device_id={"member": d}, device_id_type=MESH,
        )

    for k in far_first:

        @pl.when(peer(k) < NM - 1)
        def _():
            east_copy(k, True).start()

    own = pl.ds(pl.multiple_of(me * LOC, LOC), LOC)
    for f in range(2):
        xf[f, own, :] = pk[1 + f, 1 + me, :, :]

    @pl.when(me < NM - 1)
    def _():
        rh[2, own, :] = pk[0, me + 2, :, :]

    with jax.named_scope("obs01"):

        @pl.loop(0, 8)
        def _(g):
            for k in range(1, NM):
                obs_copy(g, k, False).wait_recv()

    odd = lax.rem(lat, 2)
    first_peer = lax.rem(lat + NL - 1 + 2 * odd, NL)
    second_peer = lax.rem(lat + NL + 1 - 2 * odd, NL)
    odd_f = odd.astype(F32)
    shifts = (2.0 * odd_f - 1.0, 1.0 - 2.0 * odd_f, 0.0)
    insides = (
        in_north * (1.0 - odd_f) + in_south * odd_f,
        in_south * (1.0 - odd_f) + in_north * odd_f,
        1.0,
    )
    c_at = iota((1, CELLS), 1)
    row_of = (c_at >> 5).astype(F32)
    col_of = (c_at & 31).astype(F32)

    def remote_gram(a, src, dst, n):
        return pltpu.make_async_remote_copy(
            src_ref=src, dst_ref=dst, send_sem=g_send.at[a, n], recv_sem=g_recv.at[a, n],
            device_id={"lat": first_peer if a == 0 else second_peer}, device_id_type=MESH,
        )

    low, top = slice(128, 256), slice(0, 128)
    has_far = has_north & has_south

    def towards(a, act):
        if a == 0:
            pl.when(has_far)(act)
        else:
            act()

    @pl.when((lat == 0) | (lat == NL - 1))
    def _():
        gr[0] = jnp.zeros((3, 256, 256), F32)
        dr[0] = jnp.zeros((8, ENS), F32)

    def gram_copies(a, n):
        if n == 1:
            return [remote_gram(a, gs.at[a, 1], gr.at[a, 1], 2)]
        at = 0 if n == 0 else 3
        return [
            remote_gram(a, gs.at[a, n, top, :], gr.at[a, n, top, :], at),
            remote_gram(a, gs.at[a, n, low, low], gr.at[a, n, low, low], at + 1),
        ]

    def drive_copy(a):
        return remote_gram(a, ds_.at[a], dr.at[a], 5)

    def member_mean(b):
        co[b, 2:3, :] = jnp.sum(rh[b], axis=0, keepdims=True) * (1.0 / ENS)

    def weigh(a, b, to_h, to_l, at):
        up = ((row_of - shifts[a] * ROWS) - 0.5 * (ROWS - 1)) / ROWS
        east = ((col_of + (b - 1) * 32) - 0.5 * 31) / 32
        t_root = jnp.exp(-0.25 * (up * up + east * east)) * insides[a]
        s_w = t_root * co[b, 0:1, :]
        y_bar = co[b, 2:3, :]

        @pl.loop(0, ENS // 64)
        def _(n):
            r = pl.ds(pl.multiple_of(n * 64, 64), 64)
            s_h, s_l = split((rh[b, r, :] - y_bar) * s_w)
            to_h[r, at : at + CELLS] = s_h
            to_l[r, at : at + CELLS] = s_l

        return t_root * (co[b, 1:2, :] - y_bar * co[b, 0:1, :])

    def products(h, l):
        left, right = slice(0, 256), slice(256, 512)
        first = dot(h[left, :], h[left, :], NT) + dot(h[left, :], l[left, :], NT)
        first = first + dot(l[left, :], h[left, :], NT)
        both = dot(h[...], h[right, :], NT) + dot(h[...], l[right, :], NT)
        both = both + dot(l[...], h[right, :], NT)
        return [first, both[left], both[right]]

    for b in range(2):
        member_mean(b)
    drives = []
    def west(a):
        push = [weigh(a, b, sh, sl, b * CELLS) for b in range(2)]
        for n, v in enumerate(products(sh, sl)):
            if a < 2:
                gs[a, n] = v
            else:
                g0[n] = v
        return row_times(jnp.concatenate(push, axis=1), sh[...], sl[...], NT)

    def east(a):
        push = weigh(a, 2, s2h, s2l, 0)
        left, right = slice(0, 256), slice(256, 512)

        def keep(n, v):
            if a == 2:
                g0[n] = g0[n] + v
                return
            gs[a, n] = gs[a, n] + v

            def send():
                for c in gram_copies(a, n):
                    c.start()

            towards(a, send)

        first = dot(s2h[left, :], s2h[left, :], NT) + dot(s2h[left, :], s2l[left, :], NT)
        keep(0, first + dot(s2l[left, :], s2h[left, :], NT))
        both = dot(s2h[...], s2h[right, :], NT) + dot(s2h[...], s2l[right, :], NT)
        both = both + dot(s2l[...], s2h[right, :], NT)
        keep(1, both[left])
        keep(2, both[right])
        return row_times(push, s2h[...], s2l[...], NT)

    drives = [None] * 3
    with jax.named_scope("gram01"):
        for a in range(2):
            drives[a] = west(a)

    with jax.named_scope("obs2"):

        @pl.when(me < NM - 1)
        def _():
            for k in range(1, NM):
                east_copy(k, False).wait_recv()

    member_mean(2)
    with jax.named_scope("gram2"):
        for a in range(2):
            drives[a] = drives[a] + east(a)
            ds_[a] = jnp.broadcast_to(drives[a], (8, ENS))
            towards(a, lambda a=a: drive_copy(a).start())

    with jax.named_scope("gramown"):
        drives[2] = west(2)
        drives[2] = drives[2] + east(2)

    def take_states(f):
        ref = rh.at[1] if f == 0 else xf.at[f - 1]
        if f == 0:
            bar = co[1, 2:3, :]
        else:
            bar = jnp.sum(ref[...], axis=0, keepdims=True) * (1.0 / ENS)
        bs[0:1, f * CELLS : (f + 1) * CELLS] = bar

        @pl.loop(0, ENS // 64)
        def _(n):
            r = pl.ds(pl.multiple_of(n * 64, 64), 64)
            x_h, x_l = split(ref[r, :] - bar)
            xh[r, f * CELLS : (f + 1) * CELLS] = x_h
            xl[r, f * CELLS : (f + 1) * CELLS] = x_l

    take_states(0)
    with jax.named_scope("gwait"):
        for a in range(2):

            def arrive(a=a):
                for n in range(3):
                    for c in gram_copies(a, n):
                        c.wait_recv()
                drive_copy(a).wait_recv()

            towards(a, arrive)
    for k in far_first:
        field_copy(k, True).start()
    drive = drives[2] + dr[0, 0:1, :] + dr[1, 0:1, :]

    squares = jnp.zeros((8, 128), F32)
    for n, (i, j) in enumerate(BLOCKS):
        for part in range(4):
            if i == j and part >= 2:
                lanes = ((part * 64, 128),)
            else:
                lanes = ((0, 0), (0, 128))
            for _unused, c0 in lanes:
                r, c = slice(part * 64, (part + 1) * 64), slice(c0, c0 + 128)
                tot = g0[n, r, c] + gr[0, n, r, c] + gr[1, n, r, c]
                if i == j:
                    on = iota((64, 128), 0) + part * 64 == iota((64, 128), 1) + c0
                    tot = tot + jnp.where(on, ENS - 1.0, 0.0)
                g0[n, r, c] = tot
                sq = jnp.sum((tot * tot).reshape(8, 8, 128), axis=0)
                twice = i != j or (part < 2 and c0 == 128)
                squares = squares + (2.0 * sq if twice else sq)
        if i == j:
            g0[n, low, top] = g0[n, top, low].T
    fro = jnp.sqrt(jnp.sum(squares, axis=(0, 1), keepdims=True))
    inv_fro = 1.0 / fro

    def span(i):
        return slice(i * 256, (i + 1) * 256)

    def put(h, l, i, j, v):
        v_h, v_l = split(v)
        h[span(i), span(j)] = v_h
        l[span(i), span(j)] = v_l
        if i < j:
            h[span(j), span(i)] = v_h.T
            l[span(j), span(i)] = v_l.T

    def mul(a_h, a_l, b_h, b_l, i, j):
        acc = dot(a_h[span(i), :], b_h[:, span(j)]) + dot(a_h[span(i), :], b_l[:, span(j)])
        return acc + dot(a_l[span(i), :], b_h[:, span(j)])

    def eye(i, j, scale):
        if i != j:
            return 0.0
        return jnp.where(iota((256, 256), 0) == iota((256, 256), 1), scale, 0.0)

    def square(a_h, a_l):
        for i, j in BLOCKS:
            m = mf[span(i), span(j)]
            m2 = mul(a_h, a_l, a_h, a_l, i, j)
            put(bh, bl, i, j, m2)
            put(qh, ql, i, j, 0.0625 * m2 - 0.5625 * m)
            rf[span(i), span(j)] = (1.6875 * m2 - 2.4375 * m) + eye(i, j, 2.25)

    def pair_factor(to_h, to_l):
        for i, j in BLOCKS:
            put(to_h, to_l, i, j, rf[span(i), span(j)] + mul(bh, bl, qh, ql, i, j))

    def times(to_h, to_l, a_h, a_l, b_h, b_l):
        new = [mul(a_h, a_l, b_h, b_l, i, j) for i, j in BLOCKS]
        for (i, j), v in zip(BLOCKS, new):
            put(to_h, to_l, i, j, v)

    for n, (i, j) in enumerate(BLOCKS):
        scaled = g0[n] * inv_fro
        mf[span(i), span(j)] = scaled
        put(yh, yl, i, j, scaled)
    square(yh, yl)
    pair_factor(zh, zl)
    times(yh, yl, yh, yl, zh, zl)

    def step():
        for i, j in BLOCKS:
            m = mul(zh, zl, yh, yl, i, j)
            mf[span(i), span(j)] = m
            put(mh, ml, i, j, m)
        square(mh, ml)
        pair_factor(gh, gl)

    with jax.named_scope("ns"):

        @pl.loop(0, 4)
        def _(n):
            step()
            times(yh, yl, yh, yl, gh, gl)
            times(zh, zl, gh, gl, zh, zl)

    with jax.named_scope("fields"):
        for k in range(1, NM):
            field_copy(k, False).wait_recv()
    with jax.named_scope("states"):
        for f in range(1, 3):
            take_states(f)

    with jax.named_scope("ns5"):
        step()
        times(zh, zl, gh, gl, zh, zl)
    scale = math.sqrt(ENS - 1.0) / jnp.sqrt(fro)

    def analysis_copy(k, mine):
        d = peer(k)
        owner = me if mine else source(k)
        return pltpu.make_async_remote_copy(
            src_ref=ao.at[:, pl.ds(pl.multiple_of(d * LOC, LOC), LOC), :],
            dst_ref=ro.at[:, owner, :, :],
            send_sem=a_send.at[0, k], recv_sem=a_recv.at[0, k],
            device_id={"member": d}, device_id_type=MESH,
        )

    def analysed(d, e):
        r = [pl.ds(pl.multiple_of(i * LOC, LOC), LOC) for i in (d, e)]
        high = jnp.concatenate([zh[i, :] for i in r], axis=0)
        both = dot(jnp.concatenate([high] + [zl[i, :] for i in r], axis=0), xh[...])
        acc = both[0 : 2 * LOC] + both[2 * LOC : 4 * LOC] + dot(high, xl[...])
        return acc * scale

    def bias_copy(k, mine):
        d = peer(k)
        owner = me if mine else source(k)
        return pltpu.make_async_remote_copy(
            src_ref=bd, dst_ref=bo.at[owner],
            send_sem=a_send.at[1, k], recv_sem=a_recv.at[1, k],
            device_id={"member": d}, device_id_type=MESH,
        )


    for pair in ((4, 2), (6, 3), (5, 1), (7, 0)):
        res = analysed(*(peer(k) for k in pair))
        for n, k in enumerate(pair):
            for f in range(3):
                part = res[n * LOC : (n + 1) * LOC, f * CELLS : (f + 1) * CELLS]
                if k:
                    ao[f, pl.ds(pl.multiple_of(peer(k) * LOC, LOC), LOC), :] = part
                else:
                    ro[f, me, :, :] = part
            if k:
                analysis_copy(k, True).start()
    mean_weight = row_times(row_times(drive, zh[...], zl[...]), zh[...], zl[...]) * inv_fro
    bias = bs[0:1, :] + row_times(mean_weight, xh[...], xl[...])
    lines = [bias[:, i * 128 : (i + 1) * 128] for i in range(6)]
    packed = jnp.concatenate(lines + [jnp.zeros((2, 128), F32)], axis=0)
    bd[...] = packed
    bo[me] = packed
    for k in far_first:
        bias_copy(k, True).start()
    with jax.named_scope("out"):
        for k in range(1, NM):
            analysis_copy(k, False).wait_recv()
            bias_copy(k, False).wait_recv()

    @pl.loop(0, 8)
    def _(g):

        by_relay = lax.rem(g, 2) == 1

        @pl.when(has_north & jnp.logical_not((lat == NL // 2) & by_relay))
        def _():
            halo(0, g).wait_send()

        @pl.when(has_south & jnp.logical_not((lat == NL // 2 - 1) & by_relay))
        def _():
            halo(1, g).wait_send()

        @pl.when(at_middle & by_relay)
        def _():
            detour(0, g).wait_send()

        @pl.when(at_edge & by_relay)
        def _():
            relay(0, g).wait_send()

        for k in range(1, NM):
            obs_copy(g, k, True).wait_send()

    for k in range(1, NM):

        @pl.when(peer(k) < NM - 1)
        def _():
            east_copy(k, True).wait_send()

    for k in range(1, NM):
        field_copy(k, True).wait_send()
        analysis_copy(k, True).wait_send()
        bias_copy(k, True).wait_send()
    for a in range(2):

        def left(a=a):
            for n in range(3):
                for c in gram_copies(a, n):
                    c.wait_send()
            drive_copy(a).wait_send()

        towards(a, left)


def unpack(ro, bo, out, held, sem):
    lane1 = iota((8, 128), 1)
    halves = lane1 < 64
    evens = (lane1 & 32) == 0

    def leave(g):
        rows = pl.ds(pl.multiple_of(g * 8, 8), 8)
        return pltpu.make_async_copy(held.at[:, rows], out.at[:, rows], sem.at[g])

    @pl.loop(0, 8)
    def _(g):
        rows = pl.ds(pl.multiple_of(g * 8, 8), 8)
        for f in range(3):
            for t in range(2):
                for rg in range(2):
                    at = 2 * f + rg
                    v = [
                        ro[f, 4 * t + b, rows, rg * 128 : (rg + 1) * 128]
                        + bo[4 * t + b, at : at + 1, :]
                        for b in range(4)
                    ]
                    o = exchange_lanes(v, halves, evens)
                    for j in range(4):
                        held[f, rows, rg * 4 + j, t * 128 : (t + 1) * 128] = o[j]
        leave(g).start()

    for g in range(8):
        leave(g).wait()


def body(ensemble_state, obs_cell, obs_value, obs_prec):
    vmem = pl.BlockSpec(memory_space=pltpu.VMEM)
    anywhere = pl.BlockSpec(memory_space=pltpu.HBM)
    half = pltpu.VMEM((ENS, ENS), BF16)
    full = pltpu.VMEM((ENS, ENS), F32)
    dma = pltpu.SemaphoreType.DMA
    received, biases = pl.pallas_call(
        kernel,
        out_shape=(
            jax.ShapeDtypeStruct((3, NM, LOC, CELLS), F32),
            jax.ShapeDtypeStruct((NM, 8, 128), F32),
        ),
        in_specs=[anywhere] * 4,
        out_specs=(vmem, vmem),
        scratch_shapes=[
            pltpu.VMEM((3, LOC, ROWS, LON), F32),
            pltpu.VMEM((8, 256), jnp.int32),
            pltpu.VMEM((8, 256), F32),
            pltpu.VMEM((8, 256), F32),
            pltpu.VMEM((3, ROWS, LOC, LON), F32),
            pltpu.VMEM((3, 4, LOC, LON), F32),
            pltpu.VMEM((3, 4, LOC, LON), F32),
            pltpu.VMEM((3, 4, LOC, LON), F32),
            pltpu.VMEM((3, 10, LOC, CELLS), F32),
            pltpu.VMEM((3, ENS, CELLS), F32),
            pltpu.VMEM((2, ENS, CELLS), F32),
            pltpu.VMEM((ENS, 512), BF16),
            pltpu.VMEM((ENS, 512), BF16),
            pltpu.VMEM((ENS, 256), BF16),
            pltpu.VMEM((ENS, 256), BF16),
            pltpu.VMEM((3, 256, 256), F32),
            pltpu.VMEM((2, 3, 256, 256), F32),
            pltpu.VMEM((2, 3, 256, 256), F32),
            pltpu.VMEM((2, 8, ENS), F32),
            pltpu.VMEM((2, 8, ENS), F32),
            pltpu.VMEM((3, 8, CELLS), F32),
        ]
        + [half] * 12
        + [full] * 2
        + [
            pltpu.VMEM((ENS, 768), BF16),
            pltpu.VMEM((ENS, 768), BF16),
            pltpu.VMEM((3, ENS, CELLS), F32),
            pltpu.VMEM((8, 768), F32),
            pltpu.VMEM((8, 128), F32),
            dma((11,)),
            dma((2, 8)),
            dma((2, 8)),
            dma((8,)),
            dma((8,)),
            dma((8,)),
            dma((9, 8)),
            dma((9, 8)),
            dma((8,)),
            dma((8,)),
            dma((2, 6)),
            dma((2, 6)),
            dma((2, 8)),
            dma((2, 8)),
        ],
        compiler_params=pltpu.CompilerParams(
            collective_id=0, has_side_effects=True, vmem_limit_bytes=40 << 20
        ),
        name="letkf_cycle",
    )(*(pltpu.with_memory_space_constraint(a, pltpu.HBM) for a in (ensemble_state, obs_cell, obs_value, obs_prec)))
    return pl.pallas_call(
        unpack,
        out_shape=jax.ShapeDtypeStruct((3, LOC, ROWS, LON), F32),
        in_specs=[vmem, vmem],
        out_specs=pl.BlockSpec(memory_space=pl.ANY),
        scratch_shapes=[pltpu.VMEM((3, LOC, ROWS, LON), F32), dma((8,))],
        compiler_params=pltpu.CompilerParams(vmem_limit_bytes=16 << 20),
        name="unpack",
    )(received, biases)


def solution(mesh):
    in_specs = (P(None, "member", "lat", None), P(), P(), P())
    out_specs = P(None, "member", "lat", None)
    return jax.shard_map(body, mesh=mesh, in_specs=in_specs, out_specs=out_specs, check_vma=False)
```
